128 devices in a mesh: seq: 64 (over y, x_hi, z, core), dp: 2 (over x_lo).
Axes of the slice: x: 4 (x_hi: 2, x_lo: 2; x = x_hi * 2 + x_lo), y: 4, z: 4, core: 2. Of those that a mesh axis runs over, the one named last changes fastest.
Arguments:
- acceptors: bfloat16 [2, 8192, 2560], P('dp', 'seq'), may hold values from -2 to 2
- lookups: bfloat16 [2, 8192, 2560], P('dp', 'seq'), may hold values from -0.3125 to 0.3125
- payloads: bfloat16 [2, 8192, 2560], P('dp', 'seq'), may hold values from -6 to 6
- lagged_fading_source: bfloat16 [2, 8192, 2560], P('dp', 'seq'), may hold values from -6 to 6
- response_cotangent: bfloat16 [2, 8192, 2560], P('dp', 'seq'), may hold values from -2.5 to 2.5
- fading_lowering_array: bfloat16 [2560, 128], replicated, may hold values from -0.125 to 0.125
- fading_raising_array: bfloat16 [2560, 128], replicated, may hold values from -1.25 to 1.25
- feature_fading_speed: float32 [2560], replicated, may hold values from 5.812872e-06 to 0.125
- present_reward: float32 [2560], replicated, may hold values from 2.828427 to 22.627417
Outputs:
- mixed: bfloat16 [2, 8192, 2560], P('dp', 'seq')
- grad_receptance: bfloat16 [2, 8192, 2560], P('dp', 'seq')
- lookup_deriv: bfloat16 [2, 8192, 2560], P('dp', 'seq')
- payload_deriv: bfloat16 [2, 8192, 2560], P('dp', 'seq')
- grad_decay_input: bfloat16 [2, 8192, 2560], P('dp', 'seq')
- grad_lora_a: float32 [2560, 128], P('dp')
- grad_lora_b: float32 [2560, 128], P('dp')
- grad_time_decay: float32 [2560], P('dp')
- present_reward_deriv: float32 [2560], P('dp')
The draws below stay inside these ranges and needn't reach their ends.
All inputs are finite; a program needn't handle non-finite values.
Results may differ from the reference program's by a relative error of at most 0.006.
Values sent between devices are 32-bit elements.
No kernel may reach another device: no remote copies, remote signals or barrier semaphores. Data moves between devices by JAX's collectives and lax.ppermute only.
A program may use at most 320 MiB of HBM per device.

```python
import math
import jax
import jax.numpy as jnp
from jax import lax

ATTENDER_TOTAL = 40
LANE_TOTAL = 64
DECAY_RANK = 128
BLOCK = 64
EMBED_SPAN = 2560
SEQLEN = 8192
SEQS = 2


def draw_feature_fading_speed(key, part):
    choose_key, slow_key, fast_key, corner_key = jax.random.split(jax.random.fold_in(key, 7), 4)
    slower = jnp.exp(jax.random.uniform(slow_key, (EMBED_SPAN,), jnp.float32, math.log(0.05), math.log(0.6))) / SEQLEN
    faster = 1.0 / jax.random.uniform(fast_key, (EMBED_SPAN,), jnp.float32, 8.0, 40.0)
    lasting = jax.random.uniform(choose_key, (EMBED_SPAN,), jnp.float32) < 0.5
    rates = jnp.where(lasting, slower, faster)
    return jnp.clip(rates, 0.05 / SEQLEN, 0.125).astype(jnp.float32)


def block_levels(own_key, shape, cuts, low, high):
    def one(dim, parts):
        heights = jax.random.uniform(jax.random.fold_in(jax.random.fold_in(own_key, 6), dim), (parts,), jnp.float32, low / len(cuts), high / len(cuts))
        return jnp.repeat(jnp.exp(heights), shape[dim] // parts).reshape((-1,) + (1,) * (len(shape) - dim - 1))

    factor_of = one(*cuts[0])
    for cut in cuts[1:]:
        factor_of = factor_of * one(*cut)
    return factor_of


def centred(own_key, dims, spread, limit, pieces=(), dtype=jnp.bfloat16):
    array = jax.random.normal(own_key, dims, jnp.float32) * spread
    if len(pieces) > 0:
        array = block_levels(own_key, dims, pieces, -0.22, 0.18) * array
    return jnp.clip(array, min=-limit, max=limit).astype(dtype)


def setup_inputs(seed: int = 0) -> dict:
    key_list = jax.random.split(jax.random.key(seed), 10)
    acceptors = centred(key_list[0], (SEQS, SEQLEN, EMBED_SPAN), (LANE_TOTAL ** -0.5), 2.0, ((0, 2), (1, 64)))
    lookups = centred(key_list[1], (SEQS, SEQLEN, EMBED_SPAN), (2.0 / SEQLEN ** 0.5), 0.3125, ((0, 2), (1, 64)))
    payloads = centred(key_list[2], (SEQS, SEQLEN, EMBED_SPAN), 1.0, 6.0, ((0, 2), (1, 64)))
    lagged_fading_source = centred(key_list[3], (SEQS, SEQLEN, EMBED_SPAN), 1.0, 6.0, ((0, 2), (1, 64)))
    response_cotangent = centred(key_list[4], (SEQS, SEQLEN, EMBED_SPAN), (16.0 / SEQLEN ** 0.5), 2.5, ((0, 2), (1, 64)))
    fading_lowering_array = centred(key_list[5], (EMBED_SPAN, DECAY_RANK), EMBED_SPAN ** -0.5, 0.125)
    fading_raising_array = centred(key_list[6], (EMBED_SPAN, DECAY_RANK), 0.08, 1.25)
    feature_fading_speed = draw_feature_fading_speed(jax.random.fold_in(key_list[9], 71), 0)
    present_reward = jnp.clip(jnp.exp(jax.random.uniform(key_list[8], (EMBED_SPAN,), jnp.float32, math.log(2.828427), math.log(22.627417))), 2.828427, 22.627417)
    return dict(acceptors=acceptors, lookups=lookups, payloads=payloads, lagged_fading_source=lagged_fading_source, response_cotangent=response_cotangent, fading_lowering_array=fading_lowering_array, fading_raising_array=fading_raising_array, feature_fading_speed=feature_fading_speed, present_reward=present_reward)


HIGH = lax.Precision.HIGHEST


def contract(pattern, left, right):
    return jnp.einsum(pattern, left, right, precision=HIGH, preferred_element_type=jnp.float32)


def decay_log_values(input_rows, fading_lowering_array, fading_raising_array, feature_fading_speed):
    apply_projection = jnp.dot(input_rows, fading_lowering_array, preferred_element_type=jnp.float32)
    smoothed_values = jnp.tanh(apply_projection)
    gate_portion = smoothed_values.astype(jnp.bfloat16)
    rank_projection = lax.dot_general(gate_portion, fading_raising_array, (((1,), (1,)), ((), ())), preferred_element_type=jnp.float32)
    return smoothed_values, gate_portion, -feature_fading_speed[None, :] * jnp.exp(rank_projection)


def compose(decays, own_states, backward):
    def advance(carry, member):
        run_decay, run_state = carry
        decay, own_state = member
        return (run_decay * decay, decay[..., None] * run_state + own_state), carry

    initial = (jnp.ones(decays.shape[1:], jnp.float32), jnp.zeros(own_states.shape[1:], jnp.float32))
    return lax.scan(advance, initial, (decays, own_states), reverse=backward)


def temporal_blend_sublevel(acceptor_lines, lookups, payloads, incoming_cotangent, fading_exponent, reward_by_attender, adjacent_shardlink):
    inclusive = jnp.cumsum(fading_exponent, axis=1)
    exclusive = inclusive - fading_exponent
    middle = inclusive[:, BLOCK // 2 - 1:BLOCK // 2]
    overall = inclusive[:, -1]
    entering = jnp.exp(exclusive)
    leaving = jnp.exp(overall[:, None] - inclusive)
    upward = jnp.exp(exclusive - middle)
    downward = jnp.exp(middle - inclusive)
    decays = jnp.exp(overall)
    reached = acceptor_lines * entering
    faded_keys = lookups * leaving
    own_states = contract("nchk,nchv->nhkv", faded_keys, payloads)
    pull_states = contract("nchk,nchv->nhkv", reached, incoming_cotangent)
    starts, block_ends = adjacent_shardlink(decays, own_states, pull_states)
    position = jnp.arange(BLOCK)
    beneath = position[:, None] > position[None, :]
    early_recept = acceptor_lines * upward
    late_keys = lookups * downward
    scores = jnp.where(beneath, contract("nthk,nshk->nhts", early_recept, late_keys), 0.0)
    present_contribution = jnp.sum(acceptor_lines * reward_by_attender * lookups, axis=-1)[..., None]
    blended_response = contract("nhts,nshv->nthv", scores, payloads) + present_contribution * payloads + contract("nthk,nhkv->nthv", reached, starts)
    grad_start = decays[..., None] * block_ends + pull_states
    products = jnp.where(beneath, contract("nthv,nshv->nhts", incoming_cotangent, payloads), 0.0)
    agreement_verify = jnp.sum(payloads * incoming_cotangent, axis=-1)[..., None]
    memory_acceptors = entering * contract("nhkv,nthv->nthk", starts, incoming_cotangent) + upward * contract("nhts,nshk->nthk", products, late_keys)
    memory_lookup_lines = leaving * contract("nhkv,nthv->nthk", block_ends, payloads) + downward * contract("nhst,nshk->nthk", products, early_recept)
    payload_deriv = contract("nthk,nhkv->nthv", faded_keys, block_ends) + contract("nhst,nshv->nthv", scores, incoming_cotangent) + present_contribution * incoming_cotangent
    acceptor_deriv = memory_acceptors + reward_by_attender * lookups * agreement_verify
    lookup_deriv = memory_lookup_lines + reward_by_attender * acceptor_lines * agreement_verify
    present_reward_deriv = jnp.sum(acceptor_lines * lookups * agreement_verify, axis=(0, 1))
    coupling = jnp.sum(grad_start * starts, axis=-1)
    change = lookups * memory_lookup_lines - acceptor_lines * memory_acceptors
    fading_deriv = coupling[:, None] + jnp.cumsum(change, axis=1) - change - acceptor_lines * memory_acceptors
    return blended_response, acceptor_deriv, lookup_deriv, payload_deriv, fading_deriv, present_reward_deriv


def sublevel_evaluation(reshaped_acceptors, reshaped_lookups, reshaped_payloads, reshaped_source, incoming_cotangent_reshaped, fading_lowering_array, fading_raising_array, feature_fading_speed, present_reward, adjacent_shardlink):
    smoothed_values, gate_portion, fading_exponent = decay_log_values(reshaped_source, fading_lowering_array, fading_raising_array, feature_fading_speed)
    tokens, feature_span = reshaped_acceptors.shape
    tiling_arrangement = (tokens // BLOCK, BLOCK, ATTENDER_TOTAL, LANE_TOTAL)
    collected_outcomes = temporal_blend_sublevel(reshaped_acceptors.astype(jnp.float32).reshape(tiling_arrangement),
                       reshaped_lookups.astype(jnp.float32).reshape(tiling_arrangement),
                       reshaped_payloads.astype(jnp.float32).reshape(tiling_arrangement),
                       incoming_cotangent_reshaped.astype(jnp.float32).reshape(tiling_arrangement),
                       fading_exponent.reshape(tiling_arrangement), present_reward.reshape(ATTENDER_TOTAL, LANE_TOTAL), adjacent_shardlink)
    blended_response, acceptor_deriv, lookup_deriv, payload_deriv, fading_deriv, present_reward_deriv = collected_outcomes
    slope = fading_deriv.reshape(tokens, feature_span) * fading_exponent
    slope_portion = slope.astype(jnp.bfloat16)
    gate_gradient = jnp.dot(slope_portion, fading_raising_array, preferred_element_type=jnp.float32)
    projection_gradient = (gate_gradient * (1.0 - smoothed_values * smoothed_values)).astype(jnp.bfloat16)
    input_gradient = lax.dot_general(projection_gradient, fading_lowering_array, (((1,), (1,)), ((), ())), preferred_element_type=jnp.float32).astype(jnp.bfloat16)
    lowering_array_deriv = lax.dot_general(reshaped_source, projection_gradient, (((0,), (0,)), ((), ())), preferred_element_type=jnp.float32)
    raising_array_deriv = lax.dot_general(slope_portion, gate_portion, (((0,), (0,)), ((), ())), preferred_element_type=jnp.float32)
    speed_deriv = jnp.sum(slope, axis=0)

    def flatten(member):
        return member.reshape(tokens, feature_span).astype(jnp.bfloat16)

    return (flatten(blended_response), flatten(acceptor_deriv), flatten(lookup_deriv), flatten(payload_deriv), input_gradient,
            (lowering_array_deriv, raising_array_deriv, speed_deriv, present_reward_deriv.reshape(feature_span)))


def sharded_ownlink(decays, own_states, pull_states):
    ahead_total, ahead = compose(decays, own_states, False)
    behind_total, behind = compose(decays, pull_states, True)
    return ahead[1], behind[1]


def reference(acceptors, lookups, payloads, lagged_fading_source, response_cotangent, fading_lowering_array, fading_raising_array, feature_fading_speed, present_reward):
    collected = []
    for symbol_stream in range(acceptors.shape[0]):
        collected.append(sublevel_evaluation(acceptors[symbol_stream], lookups[symbol_stream], payloads[symbol_stream], lagged_fading_source[symbol_stream],
                                    response_cotangent[symbol_stream], fading_lowering_array, fading_raising_array, feature_fading_speed, present_reward, sharded_ownlink))
    stacked = [jnp.stack([member[index] for member in collected]) for index in range(5)]
    summed = [jnp.sum(jnp.stack([member[5][index] for member in collected]), axis=0) for index in range(4)]
    return (stacked[0], stacked[1], stacked[2], stacked[3], stacked[4], summed[0], summed[1], summed[2], summed[3])
```

```python
import functools
import jax
import jax.numpy as jnp
from jax import lax
from jax.experimental import pallas as pl
from jax.experimental.pallas import tpu as pltpu
from jax.sharding import Mesh
from jax.sharding import PartitionSpec as P

LANE_TOTAL = 64
BLOCK = 64
TOKENS = 128
PAIRS = 20
SPAN = 2560
SEQ = ("seq_0", "seq_1", "seq_2", "seq_3")
F32 = jnp.float32
BF16 = jnp.bfloat16
NN = (((1,), (0,)), ((), ()))
NT = (((1,), (1,)), ((), ()))
TN = (((0,), (0,)), ((), ()))


def mm(left, right, dims):
    return lax.dot_general(left, right, dims, preferred_element_type=F32)


def iotas():
    rows = lax.broadcasted_iota(jnp.int32, (TOKENS, 128), 0)
    cols = lax.broadcasted_iota(jnp.int32, (TOKENS, 128), 1)
    return rows, cols


def parts3(x):
    hi = x.astype(BF16)
    rest = x - hi.astype(F32)
    mid = rest.astype(BF16)
    low = (rest - mid.astype(F32)).astype(BF16)
    return hi, mid, low


def sum_rows(matrix, x):
    hi, mid, low = parts3(x)
    return mm(matrix, hi, NN) + mm(matrix, mid, NN) + mm(matrix, low, NN)


def per_block(row_of, first):
    top = jnp.broadcast_to(row_of[first : first + 1], (BLOCK, 128))
    bottom = jnp.broadcast_to(row_of[BLOCK + first : BLOCK + first + 1], (BLOCK, 128))
    return jnp.concatenate([top, bottom], axis=0)


def pack(full, low_lanes):
    return jnp.where(low_lanes, full[:LANE_TOTAL], full[LANE_TOTAL:])


def early_kernel(x_ref, r_ref, k_ref, v_ref, g_ref, down_ref, up_ref, speed_ref,
                 send_ref, smooth_ref, log_ref, inc_ref, own_ref, pull_ref):
    project = mm(x_ref[...], down_ref[...], NN)
    smooth = jnp.tanh(project)
    smooth_ref[...] = smooth
    gate = smooth.astype(BF16)
    rows, cols = iotas()
    lower = ((rows >= cols) & (rows // BLOCK == cols // BLOCK)).astype(F32).astype(BF16)
    low_lanes = cols[:LANE_TOTAL] < LANE_TOTAL

    def pair(p, carry):
        lanes = pl.ds(pl.multiple_of(p * 128, 128), 128)
        rank = mm(gate, up_ref[lanes, :], NT)
        log_decay = -speed_ref[:, lanes] * jnp.exp(rank)
        inc = sum_rows(lower, log_decay)
        log_ref[:, lanes] = log_decay
        inc_ref[:, lanes] = inc
        exc = inc - log_decay
        total = per_block(inc, BLOCK - 1)
        reached = (r_ref[:, lanes].astype(F32) * jnp.exp(exc)).astype(BF16)
        faded = (k_ref[:, lanes].astype(F32) * jnp.exp(total - inc)).astype(BF16)
        v = v_ref[:, lanes]
        g = g_ref[:, lanes]
        own = [pack(mm(v[b : b + BLOCK], faded[b : b + BLOCK], TN), low_lanes) for b in (0, BLOCK)]
        pull = [pack(mm(g[b : b + BLOCK], reached[b : b + BLOCK], TN), low_lanes) for b in (0, BLOCK)]
        total_0 = inc[BLOCK - 1 : BLOCK]
        total_1 = inc[TOKENS - 1 : TOKENS]
        ahead = jnp.exp(total_1) * own[0] + own[1]
        behind = jnp.exp(total_0) * pull[1] + pull[0]
        whole = jnp.exp(total_0 + total_1)
        here = pl.ds(pl.multiple_of(p * LANE_TOTAL, LANE_TOTAL), LANE_TOTAL)
        own_ref[here, :] = own[0]
        pull_ref[0, here, :] = pull[0]
        pull_ref[1, here, :] = pull[1]
        for way, state in enumerate((ahead, behind)):
            for q in range(8):
                group = way * 160 + p * 8 + q
                slot = group // 5
                place = group % 5
                send_ref[slot, pl.ds(pl.multiple_of(place * 8, 8), 8), :] = state[q * 8 : q * 8 + 8]
                send_ref[slot, pl.ds(40 + place, 1), :] = whole
        return carry

    lax.fori_loop(0, PAIRS, pair, 0)


def scan_kernel(flip_ref, in_ref, out_ref):
    count = in_ref.shape[0]
    flip = flip_ref[0]

    def step(e, run):
        at = jnp.where(flip > 0, count - 1 - e, e)
        result = []
        for q in range(5):
            out_ref[at, q * 8 : q * 8 + 8, :] = run[q]
            decay = in_ref[at, 40 + q : 41 + q, :]
            result.append(decay * run[q] + in_ref[at, q * 8 : q * 8 + 8, :])
        return tuple(result)

    lax.fori_loop(0, count, step, tuple(jnp.zeros((8, 128), F32) for _ in range(5)))


def late_kernel(x_ref, r_ref, k_ref, v_ref, g_ref, down_ref, up_ref, bonus_ref,
                smooth_ref, log_ref, inc_ref, own_ref, pull_ref, state_ref,
                mixed_ref, gr_ref, gk_ref, gv_ref, gx_ref, send_ref):
    smooth = smooth_ref[...]
    gate = smooth.astype(BF16)
    rows, cols = iotas()
    same = rows // BLOCK == cols // BLOCK
    strict = (rows > cols) & same
    strict_2 = jnp.concatenate([strict, strict], axis=0)
    before = strict.astype(F32).astype(BF16)
    heads = ((rows // LANE_TOTAL) == (cols // LANE_TOTAL)).astype(F32).astype(BF16)
    heads_2 = jnp.concatenate([heads, heads], axis=0)
    low = cols < LANE_TOTAL
    low_lanes = low[:LANE_TOTAL]
    nothing = jnp.zeros((TOKENS, 128), BF16)
    nothing_f = jnp.zeros((LANE_TOTAL, 128), F32)

    def two(x):
        x = x.astype(F32)
        zero = jnp.zeros_like(x)
        return jnp.concatenate([jnp.where(low, x, zero), jnp.where(low, zero, x)], axis=0).astype(BF16)

    def corners(state):
        return jnp.concatenate([jnp.where(low_lanes, state, nothing_f), jnp.where(low_lanes, nothing_f, state)], axis=0).astype(BF16)

    def beside(x):
        return jnp.concatenate([x[:TOKENS], x[TOKENS:]], axis=1)

    def head_sums(x):
        hi = x.astype(BF16)
        rest = (x - hi.astype(F32)).astype(BF16)
        return mm(jnp.concatenate([hi, rest], axis=1), heads_2, NN)

    def put(base, p, tile):
        for q in range(16):
            group = base + p * 16 + q
            slot = group // 5
            place = group % 5
            send_ref[slot, pl.ds(pl.multiple_of(place * 8, 8), 8), :] = tile[q * 8 : q * 8 + 8]

    def base_of(p, second):
        half = p // (PAIRS // 2)
        return half * 320 + second * 160 - half * 160

    def pair(p, gate_grad):
        lanes = pl.ds(pl.multiple_of(p * 128, 128), 128)
        here = pl.ds(pl.multiple_of(p * LANE_TOTAL, LANE_TOTAL), LANE_TOTAL)
        there = pl.ds(pl.multiple_of(PAIRS * LANE_TOTAL + p * LANE_TOTAL, LANE_TOTAL), LANE_TOTAL)
        v = v_ref[:, lanes]
        g = g_ref[:, lanes]
        rf = r_ref[:, lanes].astype(F32)
        kf = k_ref[:, lanes].astype(F32)
        vf = v.astype(F32)
        gf = g.astype(F32)
        bonus = bonus_ref[:, lanes]
        log_decay = log_ref[:, lanes]
        inc = inc_ref[:, lanes]
        exc = inc - log_decay
        total = per_block(inc, BLOCK - 1)
        middle = per_block(inc, BLOCK // 2 - 1)
        entering = jnp.exp(exc)
        leaving = jnp.exp(total - inc)
        upward = jnp.exp(exc - middle)
        downward = jnp.exp(middle - inc)
        reached = (rf * entering).astype(BF16)
        faded = (kf * leaving).astype(BF16)
        early = (rf * upward).astype(BF16)
        late = (kf * downward).astype(BF16)
        early_2 = two(early)
        late_2 = two(late)
        v_2 = two(v)
        g_2 = two(g)
        scores = jnp.where(strict_2, mm(early_2, late, NT), 0.0).astype(BF16)
        products = jnp.where(strict_2, mm(g_2, v, NT), 0.0).astype(BF16)
        present = head_sums(rf * bonus * kf)
        agree = head_sums(vf * gf)
        decay_0 = jnp.exp(inc[BLOCK - 1 : BLOCK])
        decay_1 = jnp.exp(inc[TOKENS - 1 : TOKENS])
        start_0 = state_ref[here, :]
        end_1 = state_ref[there, :]
        start_1 = decay_0 * start_0 + own_ref[here, :]
        end_0 = decay_1 * end_1 + pull_ref[1, here, :]
        s_0, s_1, e_0, e_1 = (corners(z) for z in (start_0, start_1, end_0, end_1))

        def blocks(left, right_0, right_1, dims):
            return jnp.concatenate([mm(left[:BLOCK], right_0, dims), mm(left[BLOCK:], right_1, dims)], axis=0)

        mixed = mm(beside(scores), v_2, NN) + blocks(reached, s_0, s_1, NT) + present * vf
        mixed_ref[:, lanes] = mixed.astype(BF16)
        gv = mm(scores, g_2, TN) + blocks(faded, e_0, e_1, NT) + present * gf
        gv_ref[:, lanes] = gv.astype(BF16)
        r_start = blocks(g, s_0, s_1, NN)
        r_near = mm(beside(products), late_2, NN)
        k_end = blocks(v, e_0, e_1, NN)
        k_near = mm(products, early_2, TN)
        gr_ref[:, lanes] = (entering * r_start + upward * r_near + bonus * kf * agree).astype(BF16)
        gk_ref[:, lanes] = (leaving * k_end + downward * k_near + bonus * rf * agree).astype(BF16)
        bonus_row = jnp.sum(rf * kf * agree, axis=0, keepdims=True)
        r_part = reached.astype(F32) * r_start + early.astype(F32) * r_near
        k_part = faded.astype(F32) * k_end + late.astype(F32) * k_near

        def rounded(z):
            return z.astype(BF16).astype(F32)

        couple_0 = jnp.sum((decay_0 * rounded(end_0) + pull_ref[0, here, :]) * rounded(start_0), axis=0, keepdims=True)
        couple_1 = jnp.sum((decay_1 * rounded(end_1) + pull_ref[1, here, :]) * rounded(start_1), axis=0, keepdims=True)
        coupling = jnp.concatenate([jnp.broadcast_to(couple_0, (BLOCK, 128)), jnp.broadcast_to(couple_1, (BLOCK, 128))], axis=0)
        fading = coupling + sum_rows(before, k_part - r_part) - r_part
        slope = fading * log_decay
        slope_half = slope.astype(BF16)
        slope_row = jnp.sum(slope, axis=0, keepdims=True)
        put(base_of(p, 1), p, mm(slope_half, gate, TN))
        half = p // (PAIRS // 2)
        row_slot = half * 64 + p - half * (PAIRS // 2)
        send_ref[row_slot, 40:41, :] = slope_row
        send_ref[row_slot + PAIRS // 2, 40:41, :] = bonus_row
        return gate_grad + mm(slope_half, up_ref[lanes, :], NN)

    gate_grad = lax.fori_loop(0, PAIRS, pair, jnp.zeros((TOKENS, 128), F32))
    project_grad = (gate_grad * (1.0 - smooth * smooth)).astype(BF16)

    def tail(p, carry):
        lanes = pl.ds(pl.multiple_of(p * 128, 128), 128)
        gx_ref[:, lanes] = mm(project_grad, down_ref[lanes, :], NT).astype(BF16)
        put(base_of(p, 0), p, mm(x_ref[:, lanes], project_grad, TN))
        return carry

    lax.fori_loop(0, PAIRS, tail, 0)


def call(kernel, outs, name, flops=0):
    return pl.pallas_call(
        kernel,
        out_shape=[jax.ShapeDtypeStruct(s, d) for s, d in outs],
        compiler_params=pltpu.CompilerParams(vmem_limit_bytes=56 * 1024 * 1024),
        name=name,
    )


def per_device(r, k, v, x, g, down, up, speed, bonus):
    r, k, v, x, g = (z[0] for z in (r, k, v, x, g))
    speed = speed[None]
    bonus = bonus[None]
    wide = (TOKENS, SPAN)
    state_rows = PAIRS * LANE_TOTAL
    send, smooth, log_decay, inc, own, pull = call(
        early_kernel,
        [((64, 48, 128), F32), ((TOKENS, 128), F32), (wide, F32), (wide, F32), ((state_rows, 128), F32), ((2, state_rows, 128), F32)],
        "early",
    )(x, r, k, v, g, down, up, speed)
    got = lax.all_to_all(send, SEQ, 0, 0, tiled=True)
    flip = (lax.axis_index(SEQ) >= 32).astype(jnp.int32)[None]
    back = pl.pallas_call(
        scan_kernel,
        out_shape=jax.ShapeDtypeStruct((64, 40, 128), F32),
        in_specs=[pl.BlockSpec(memory_space=pltpu.SMEM), pl.BlockSpec(memory_space=pltpu.VMEM)],
        name="scan",
    )(flip, got)
    state = lax.all_to_all(back, SEQ, 0, 0, tiled=True).reshape(2 * state_rows, 128)
    mixed, gr, gk, gv, gx, grads = call(
        late_kernel,
        [(wide, BF16)] * 5 + [((128, 48, 128), F32)],
        "late",
    )(x, r, k, v, g, down, up, bonus, smooth, log_decay, inc, own, pull, state)
    pieces = lax.all_to_all(grads, ("dp",) + SEQ, 0, 0, tiled=True)
    mine = jnp.sum(pieces, axis=0)
    whole = lax.all_to_all(jnp.broadcast_to(mine[None], (64, 48, 128)), SEQ, 0, 0, tiled=True)
    lora_a = whole[:32, :40].reshape(SPAN // 2, 128)
    lora_b = whole[32:, :40].reshape(SPAN // 2, 128)
    rows = whole[:20, 40]
    return (mixed[None], gr[None], gk[None], gv[None], gx[None], lora_a, lora_b,
            rows[:10].reshape(SPAN // 2), rows[10:].reshape(SPAN // 2))


def solution(mesh):
    split = Mesh(mesh.devices.reshape(4, 2, 4, 2, mesh.shape["dp"]), SEQ + ("dp",))
    tokens = P("dp", SEQ, None)
    return jax.shard_map(
        per_device,
        mesh=split,
        in_specs=(tokens,) * 5 + (P(),) * 4,
        out_specs=(tokens,) * 5 + (P("dp", None), P("dp", None), P("dp"), P("dp")),
        check_vma=False,
    )
```

```python
import jax
import jax.numpy as jnp
from jax import lax
from jax.experimental import pallas as pl
from jax.experimental.pallas import tpu as pltpu
from jax.sharding import Mesh
from jax.sharding import PartitionSpec as P


LANE_TOTAL = 64
BLOCK = 64
TOKENS = 128
PAIRS = 20
SPAN = 2560
SEQ = ("seq_0", "seq_1", "seq_2", "seq_3")
CHIPS = SEQ[:3]
CORE = SEQ[3]
HALF = 10
HALF_ROWS = 640
CHUNK = 5
STEPS = 4
TAIL = 5
VMEM_LIMIT = 56
F32 = jnp.float32
BF16 = jnp.bfloat16
NN = (((1,), (0,)), ((), ()))
NT = (((1,), (1,)), ((), ()))
TN = (((0,), (0,)), ((), ()))


def mm(left, right, dims):
    return lax.dot_general(left, right, dims, preferred_element_type=F32)


def iotas():
    rows = lax.broadcasted_iota(jnp.int32, (TOKENS, 128), 0)
    cols = lax.broadcasted_iota(jnp.int32, (TOKENS, 128), 1)
    return rows, cols


def parts3(x):
    hi = x.astype(BF16)
    rest = x - hi.astype(F32)
    mid = rest.astype(BF16)
    low = (rest - mid.astype(F32)).astype(BF16)
    return hi, mid, low


def sum_rows(matrix, x):
    hi, mid, low = parts3(x)
    return mm(matrix, hi, NN) + mm(matrix, mid, NN) + mm(matrix, low, NN)


def per_block(row_of, first):
    top = jnp.broadcast_to(row_of[first : first + 1], (BLOCK, 128))
    bottom = jnp.broadcast_to(row_of[BLOCK + first : BLOCK + first + 1], (BLOCK, 128))
    return jnp.concatenate([top, bottom], axis=0)


def pack(full, low_lanes):
    return jnp.where(low_lanes, full[:LANE_TOTAL], full[LANE_TOTAL:])


def early_kernel(core_ref, x_ref, r_ref, k_ref, v_ref, g_ref, down_ref, up_ref, speed_ref,
                 theirs_ref, mine_ref, smooth_ref, log_ref, inc_ref, reached_ref, faded_ref, own_ref, pull_ref,
                 stage_ref, sems):
    step = pl.program_id(0)
    half = jnp.where(step < 2, 1 - core_ref[0], core_ref[0])

    @pl.when(step == 0)
    def _():
        smooth_ref[...] = jnp.tanh(mm(x_ref[...], down_ref[...], NN))

    gate = smooth_ref[...].astype(BF16)
    rows, cols = iotas()
    lower = ((rows >= cols) & (rows // BLOCK == cols // BLOCK)).astype(F32).astype(BF16)
    low_lanes = cols[:LANE_TOTAL] < LANE_TOTAL
    base = (step % 2) * CHUNK
    for i in range(CHUNK):
        lanes = slice(i * 128, i * 128 + 128)
        rank = mm(gate, up_ref[lanes, :], NT)
        log_decay = -speed_ref[pl.ds(half * HALF + base + i, 1), :] * jnp.exp(rank)
        inc = sum_rows(lower, log_decay)
        log_ref[:, lanes] = log_decay
        inc_ref[:, lanes] = inc
        exc = inc - log_decay
        total = per_block(inc, BLOCK - 1)
        reached = (r_ref[:, lanes].astype(F32) * jnp.exp(exc)).astype(BF16)
        faded = (k_ref[:, lanes].astype(F32) * jnp.exp(total - inc)).astype(BF16)
        reached_ref[:, lanes] = reached
        faded_ref[:, lanes] = faded
        v = v_ref[:, lanes]
        g = g_ref[:, lanes]
        own = [pack(mm(v[b : b + BLOCK], faded[b : b + BLOCK], TN), low_lanes) for b in (0, BLOCK)]
        pull = [pack(mm(g[b : b + BLOCK], reached[b : b + BLOCK], TN), low_lanes) for b in (0, BLOCK)]
        total_0 = inc[BLOCK - 1 : BLOCK]
        total_1 = inc[TOKENS - 1 : TOKENS]
        here = slice(i * LANE_TOTAL, i * LANE_TOTAL + LANE_TOTAL)
        own_ref[here, :] = own[0]
        pull_ref[0, here, :] = pull[0]
        pull_ref[1, here, :] = pull[1]
        row = pl.multiple_of((base + i) * LANE_TOTAL, LANE_TOTAL)
        stage_ref[step // 2, pl.ds(row, LANE_TOTAL), :] = jnp.exp(total_1) * own[0] + own[1]
        stage_ref[step // 2, pl.ds(HALF_ROWS + row, LANE_TOTAL), :] = jnp.exp(total_0) * pull[1] + pull[0]
        stage_ref[step // 2, pl.ds(2 * HALF_ROWS + base + i, 1), :] = jnp.exp(total_0 + total_1)

    @pl.when(step == STEPS - 1)
    def _():
        copies = [pltpu.make_async_copy(stage_ref.at[j], ref, sems.at[j]) for j, ref in enumerate((theirs_ref, mine_ref))]
        for copy in copies:
            copy.start()
        for copy in copies:
            copy.wait()


def join_kernel(place_ref, mine_ref, other_ref, send_ref):
    first = place_ref[0] == 0

    def both(rows):
        mine = mine_ref[rows, :]
        other = other_ref[rows, :]
        return jnp.where(first, mine, other), jnp.where(first, other, mine)

    for i in range(HALF):
        decay_a, decay_b = both(slice(2 * HALF_ROWS + i, 2 * HALF_ROWS + i + 1))
        decay = decay_a * decay_b
        for q in range(8):
            at = i * LANE_TOTAL + q * 8
            own_a, own_b = both(slice(at, at + 8))
            pull_a, pull_b = both(slice(HALF_ROWS + at, HALF_ROWS + at + 8))
            for way, state in enumerate((decay_b * own_a + own_b, pull_a + decay_a * pull_b)):
                group = way * 80 + i * 8 + q
                slot, place = divmod(group, 5)
                send_ref[slot, place * 8 : place * 8 + 8, :] = state
                send_ref[slot, 40 + place : 41 + place, :] = decay


def scan_kernel(place_ref, in_ref, out_ref):
    count = in_ref.shape[0]
    flip = place_ref[0]

    def step(e, run):
        at = jnp.where(flip > 0, count - 1 - e, e)
        result = []
        for q in range(5):
            out_ref[at, q * 8 : q * 8 + 8, :] = run[q]
            decay = in_ref[at, 40 + q : 41 + q, :]
            result.append(decay * run[q] + in_ref[at, q * 8 : q * 8 + 8, :])
        return tuple(result)

    lax.fori_loop(0, count, step, tuple(jnp.zeros((8, 128), F32) for _ in range(5)))


def part_kernel(place_ref, chip_ref, mine_ref, other_ref, keep_ref, give_ref):
    first = place_ref[0] == 0

    def both(rows):
        mine = mine_ref[rows, :]
        other = other_ref[rows, :]
        return jnp.where(first, mine, other), jnp.where(first, other, mine)

    for i in range(HALF):
        decay_a, decay_b = both(slice(2 * HALF_ROWS + i, 2 * HALF_ROWS + i + 1))
        ahead = slice(i * LANE_TOTAL, i * LANE_TOTAL + LANE_TOTAL)
        behind = slice(HALF_ROWS + i * LANE_TOTAL, HALF_ROWS + i * LANE_TOTAL + LANE_TOTAL)
        start_a = chip_ref[ahead, :]
        end_b = chip_ref[behind, :]
        start_b = decay_a * start_a + jnp.where(first, mine_ref[ahead, :], other_ref[ahead, :])
        end_a = decay_b * end_b + jnp.where(first, other_ref[behind, :], mine_ref[behind, :])
        keep_ref[ahead, :] = jnp.where(first, start_a, start_b)
        give_ref[ahead, :] = jnp.where(first, start_b, start_a)
        keep_ref[behind, :] = jnp.where(first, end_a, end_b)
        give_ref[behind, :] = jnp.where(first, end_b, end_a)


def two(x, low):
    x = x.astype(F32)
    zero = jnp.zeros_like(x)
    return jnp.concatenate([jnp.where(low, x, zero), jnp.where(low, zero, x)], axis=0).astype(BF16)


def corners(state, low_lanes):
    zero = jnp.zeros_like(state)
    return jnp.concatenate([jnp.where(low_lanes, state, zero), jnp.where(low_lanes, zero, state)], axis=0).astype(BF16)


def beside(x):
    return jnp.concatenate([x[:TOKENS], x[TOKENS:]], axis=1)


def blocks(left, right_0, right_1, dims):
    return jnp.concatenate([mm(left[:BLOCK], right_0, dims), mm(left[BLOCK:], right_1, dims)], axis=0)


def near_kernel(core_ref, r_ref, k_ref, v_ref, g_ref, bonus_ref, log_ref, inc_ref,
                fade_ref, mixed_ref, gr_ref, gk_ref, gv_ref, row_ref):
    rows, cols = iotas()
    same = rows // BLOCK == cols // BLOCK
    strict = (rows > cols) & same
    strict_2 = jnp.concatenate([strict, strict], axis=0)
    before = strict.astype(F32).astype(BF16)
    heads = ((rows // LANE_TOTAL) == (cols // LANE_TOTAL)).astype(F32).astype(BF16)
    heads_2 = jnp.concatenate([heads, heads], axis=0)
    low = cols < LANE_TOTAL

    def head_sums(x):
        hi = x.astype(BF16)
        rest = (x - hi.astype(F32)).astype(BF16)
        return mm(jnp.concatenate([hi, rest], axis=1), heads_2, NN)

    step = pl.program_id(0)
    for i in range(CHUNK):
        p = step * CHUNK + i
        lanes = slice(i * 128, i * 128 + 128)
        v = v_ref[:, lanes]
        g = g_ref[:, lanes]
        rf = r_ref[:, lanes].astype(F32)
        kf = k_ref[:, lanes].astype(F32)
        vf = v.astype(F32)
        gf = g.astype(F32)
        bonus = bonus_ref[pl.ds(p, 1), :]
        inc = inc_ref[:, lanes]
        exc = inc - log_ref[:, lanes]
        middle = per_block(inc, BLOCK // 2 - 1)
        upward = jnp.exp(exc - middle)
        downward = jnp.exp(middle - inc)
        early = (rf * upward).astype(BF16)
        late = (kf * downward).astype(BF16)
        early_2 = two(early, low)
        late_2 = two(late, low)
        v_2 = two(v, low)
        g_2 = two(g, low)
        scores = jnp.where(strict_2, mm(early_2, late, NT), 0.0).astype(BF16)
        products = jnp.where(strict_2, mm(g_2, v, NT), 0.0).astype(BF16)
        present = head_sums(rf * bonus * kf)
        agree = head_sums(vf * gf)
        mixed_ref[:, lanes] = mm(beside(scores), v_2, NN) + present * vf
        gv_ref[:, lanes] = mm(scores, g_2, TN) + present * gf
        r_near = mm(beside(products), late_2, NN)
        k_near = mm(products, early_2, TN)
        gr_ref[:, lanes] = upward * r_near + bonus * kf * agree
        gk_ref[:, lanes] = downward * k_near + bonus * rf * agree
        row_ref[pl.ds(p, 1), :] = jnp.sum(rf * kf * agree, axis=0, keepdims=True)
        r_part = early.astype(F32) * r_near
        k_part = late.astype(F32) * k_near
        fade_ref[:, lanes] = sum_rows(before, k_part - r_part) - r_part


def start_and_end(p, i, core, mine_ref, other_ref, own_ref, pull_ref, decay_0, decay_1):
    half = p // HALF
    row = pl.multiple_of((p - half * HALF) * LANE_TOTAL, LANE_TOTAL)
    here = slice(i * LANE_TOTAL, i * LANE_TOTAL + LANE_TOTAL)

    def of(rows):
        return jnp.where(half == core, mine_ref[rows, :], other_ref[rows, :])

    start_0 = of(pl.ds(row, LANE_TOTAL))
    end_1 = of(pl.ds(HALF_ROWS + row, LANE_TOTAL))
    start_1 = decay_0 * start_0 + own_ref[here, :]
    end_0 = decay_1 * end_1 + pull_ref[1, here, :]
    return start_0, start_1, end_0, end_1


def slope_kernel(core_ref, x_ref, v_ref, g_ref, up_ref, smooth_ref, log_ref, inc_ref, reached_ref, faded_ref, own_ref, pull_ref,
                 mine_ref, other_ref, fade_ref, row_ref, keep_ref, give_ref, project_ref, stage_ref, total_ref, sems):
    core = core_ref[0]
    step = pl.program_id(0)
    smooth = smooth_ref[...]
    gate = smooth.astype(BF16)
    rows, cols = iotas()
    strict = (rows > cols) & (rows // BLOCK == cols // BLOCK)
    before = strict.astype(F32).astype(BF16)
    low_lanes = cols[:LANE_TOTAL] < LANE_TOTAL

    def put(index, p, tile):
        half = p // HALF
        for q in range(16):
            group = (p - half * HALF) * 16 + q
            slot = group // 5 * 2 + half
            place = group % 5
            stage_ref[index, slot, pl.ds(pl.multiple_of(place * 8, 8), 8), :] = tile[q * 8 : q * 8 + 8]

    def rounded(z):
        return z.astype(BF16).astype(F32)

    gate_grad = jnp.zeros((TOKENS, 128), F32)
    for i in range(CHUNK):
        p = step * CHUNK + i
        half = p // HALF
        lanes = slice(i * 128, i * 128 + 128)
        here = slice(i * LANE_TOTAL, i * LANE_TOTAL + LANE_TOTAL)
        log_decay = log_ref[:, lanes]
        decay_0 = jnp.exp(inc_ref[BLOCK - 1 : BLOCK, lanes])
        decay_1 = jnp.exp(inc_ref[TOKENS - 1 : TOKENS, lanes])
        start_0, start_1, end_0, end_1 = start_and_end(p, i, core, mine_ref, other_ref, own_ref, pull_ref, decay_0, decay_1)
        s_0, s_1, e_0, e_1 = (corners(z, low_lanes) for z in (start_0, start_1, end_0, end_1))
        r_part = reached_ref[:, lanes].astype(F32) * blocks(g_ref[:, lanes], s_0, s_1, NN)
        k_part = faded_ref[:, lanes].astype(F32) * blocks(v_ref[:, lanes], e_0, e_1, NN)
        couple_0 = jnp.sum((decay_0 * rounded(end_0) + pull_ref[0, here, :]) * rounded(start_0), axis=0, keepdims=True)
        couple_1 = jnp.sum((decay_1 * rounded(end_1) + pull_ref[1, here, :]) * rounded(start_1), axis=0, keepdims=True)
        coupling = jnp.concatenate([jnp.broadcast_to(couple_0, (BLOCK, 128)), jnp.broadcast_to(couple_1, (BLOCK, 128))], axis=0)
        fading = coupling + sum_rows(before, k_part - r_part) - r_part + fade_ref[:, lanes]
        slope = fading * log_decay
        slope_half = slope.astype(BF16)
        put(1 - core, p, mm(slope_half, gate, TN))
        row_slot = (p - half * HALF) * 2 + half
        stage_ref[core, row_slot, 40:41, :] = jnp.sum(slope, axis=0, keepdims=True)
        stage_ref[1 - core, row_slot, 40:41, :] = row_ref[pl.ds(p, 1), :]
        gate_grad = gate_grad + mm(slope_half, up_ref[lanes, :], NN)

    @pl.when(step == 0)
    def _():
        total_ref[...] = gate_grad

    @pl.when(step > 0)
    def _():
        total_ref[...] += gate_grad

    @pl.when(step == STEPS - 1)
    def _():
        project_grad = (total_ref[...] * (1.0 - smooth * smooth)).astype(BF16)
        project_ref[...] = project_grad

        def tail(p, carry):
            lanes = pl.ds(pl.multiple_of(p * 128, 128), 128)
            put(core, p, mm(x_ref[:, lanes], project_grad, TN))
            return carry

        lax.fori_loop(0, PAIRS, tail, 0, unroll=TAIL)
        copies = [pltpu.make_async_copy(stage_ref.at[j], ref, sems.at[j]) for j, ref in enumerate((keep_ref, give_ref))]
        for copy in copies:
            copy.start()
        for copy in copies:
            copy.wait()


def last_kernel(core_ref, v_ref, g_ref, down_ref, log_ref, inc_ref, reached_ref, faded_ref, own_ref, pull_ref, mine_ref, other_ref,
                near_mixed_ref, near_gr_ref, near_gk_ref, near_gv_ref, project_ref,
                mixed_ref, gr_ref, gk_ref, gv_ref, gx_ref):
    _, cols = iotas()
    low_lanes = cols[:LANE_TOTAL] < LANE_TOTAL
    project_grad = project_ref[...]
    core = core_ref[0]
    step = pl.program_id(0)
    for i in range(CHUNK):
        p = step * CHUNK + i
        lanes = slice(i * 128, i * 128 + 128)
        inc = inc_ref[:, lanes]
        decay_0 = jnp.exp(inc[BLOCK - 1 : BLOCK])
        decay_1 = jnp.exp(inc[TOKENS - 1 : TOKENS])
        states = start_and_end(p, i, core, mine_ref, other_ref, own_ref, pull_ref, decay_0, decay_1)
        s_0, s_1, e_0, e_1 = (corners(z, low_lanes) for z in states)
        entering = jnp.exp(inc - log_ref[:, lanes])
        leaving = jnp.exp(per_block(inc, BLOCK - 1) - inc)
        mixed_ref[:, lanes] = (near_mixed_ref[:, lanes] + blocks(reached_ref[:, lanes], s_0, s_1, NT)).astype(BF16)
        gv_ref[:, lanes] = (near_gv_ref[:, lanes] + blocks(faded_ref[:, lanes], e_0, e_1, NT)).astype(BF16)
        gr_ref[:, lanes] = (near_gr_ref[:, lanes] + entering * blocks(g_ref[:, lanes], s_0, s_1, NN)).astype(BF16)
        gk_ref[:, lanes] = (near_gk_ref[:, lanes] + leaving * blocks(v_ref[:, lanes], e_0, e_1, NN)).astype(BF16)
        gx_ref[:, lanes] = mm(project_grad, down_ref[lanes, :], NT).astype(BF16)


def call(kernel, outs, count=0):
    more = {}
    if count:
        more["in_specs"] = [pl.BlockSpec(memory_space=pltpu.SMEM)] + [pl.BlockSpec(memory_space=pltpu.VMEM)] * (count - 1)
    return pl.pallas_call(
        kernel,
        out_shape=[jax.ShapeDtypeStruct(s, d) for s, d in outs],
        compiler_params=pltpu.CompilerParams(vmem_limit_bytes=8 * 1024 * 1024),
        **more,
    )


WIDE = ((TOKENS, SPAN), lambda at: pl.BlockSpec((TOKENS, CHUNK * 128), lambda s, core: (0, at(s, core))))
WEIGHT = ((SPAN, 128), lambda at: pl.BlockSpec((CHUNK * 128, 128), lambda s, core: (at(s, core), 0)))
STATE = ((PAIRS * LANE_TOTAL, 128), lambda at: pl.BlockSpec((CHUNK * LANE_TOTAL, 128), lambda s, core: (at(s, core), 0)))
STATES = ((2, PAIRS * LANE_TOTAL, 128), lambda at: pl.BlockSpec((2, CHUNK * LANE_TOTAL, 128), lambda s, core: (0, at(s, core), 0)))


def whole(*shape):
    return (shape, lambda at: pl.BlockSpec(shape, lambda s, core: (0,) * len(shape)))


def kept(*shape):
    return (shape, lambda at: pl.BlockSpec(memory_space=pl.ANY))


def in_steps(kernel, ins, outs, scratch=(), at=lambda s, core: s, flops=10 ** 9):
    return pl.pallas_call(
        kernel,
        grid_spec=pltpu.PrefetchScalarGridSpec(
            num_scalar_prefetch=1,
            grid=(STEPS,),
            in_specs=[spec(at) for _, spec in ins],
            out_specs=[spec(at) for (_, spec), _ in outs],
            scratch_shapes=list(scratch),
        ),
        out_shape=[jax.ShapeDtypeStruct(shape, dtype) for (shape, _), dtype in outs],
        compiler_params=pltpu.CompilerParams(vmem_limit_bytes=VMEM_LIMIT * 1024 * 1024, dimension_semantics=("arbitrary",)),
        cost_estimate=pl.CostEstimate(flops=flops, bytes_accessed=flops // 1000, transcendentals=0),
    )


def exchange(x, axes):
    return lax.all_to_all(x, axes, 0, 0, tiled=True)


def swap(x):
    return lax.ppermute(x, CORE, [(0, 1), (1, 0)])


def inside(r, k, v, x, g, down, up, speed, bonus):
    r, k, v, x, g = (z[0] for z in (r, k, v, x, g))
    speed = speed.reshape(PAIRS, 128)
    bonus = bonus.reshape(PAIRS, 128)
    core = lax.axis_index(CORE).astype(jnp.int32)[None]
    flip = (lax.axis_index(CHIPS) // 16).astype(jnp.int32)[None]
    rows = whole(PAIRS, 128)
    square = whole(TOKENS, 128)
    part_rows = 2 * HALF_ROWS + 16
    dma = pltpu.SemaphoreType.DMA((2,))
    theirs, mine, smooth, log_decay, inc, reached, faded, own, pull = in_steps(
        early_kernel,
        [whole(TOKENS, SPAN), WIDE, WIDE, WIDE, WIDE, whole(SPAN, 128), WEIGHT, rows],
        [(kept(part_rows, 128), F32), (kept(part_rows, 128), F32), (square, F32), (WIDE, F32), (WIDE, F32), (WIDE, BF16), (WIDE, BF16),
         (STATE, F32), (STATES, F32)],
        (pltpu.VMEM((2, part_rows, 128), F32), dma), lambda s, core: ((1 - core[0]) * 2 + s) % STEPS,
    )(core, x, r, k, v, g, down, up, speed)
    other = swap(theirs)
    (joined,) = call(join_kernel, [((32, 48, 128), F32)], 3)(core, mine, other)
    there = exchange(joined, CHIPS)
    fade, near_mixed, near_gr, near_gk, near_gv, bonus_rows = in_steps(
        near_kernel, [WIDE] * 4 + [rows, WIDE, WIDE], [(WIDE, F32)] * 5 + [(rows, F32)],
    )(core, r, k, v, g, bonus, log_decay, inc)
    (scanned,) = call(scan_kernel, [((32, 40, 128), F32)], 2)(flip, there)
    chip = exchange(scanned, CHIPS).reshape(2 * HALF_ROWS, 128)
    keep, give = call(part_kernel, [((2 * HALF_ROWS, 128), F32)] * 2, 4)(core, chip, mine, other)
    got = swap(give)
    state = whole(2 * HALF_ROWS, 128)
    held, given, project_grad = in_steps(
        slope_kernel,
        [whole(TOKENS, SPAN), WIDE, WIDE, WEIGHT, square, WIDE, WIDE, WIDE, WIDE, STATE, STATES, state, state, WIDE, rows],
        [(kept(64, 48, 128), F32), (kept(64, 48, 128), F32), (square, BF16)],
        (pltpu.VMEM((2, 64, 48, 128), F32), pltpu.VMEM((TOKENS, 128), F32), dma),
    )(core, x, v, g, up, smooth, log_decay, inc, reached, faded, own, pull, keep, got, fade, bonus_rows)
    grads = held + swap(given)
    pieces = exchange(grads, CHIPS + ("dp",))
    mixed, gr, gk, gv, gx = in_steps(
        last_kernel,
        [WIDE, WIDE, WEIGHT, WIDE, WIDE, WIDE, WIDE, STATE, STATES, state, state, WIDE, WIDE, WIDE, WIDE, square],
        [(WIDE, BF16)] * 5,
    )(core, v, g, down, log_decay, inc, reached, faded, own, pull, keep, got, near_mixed, near_gr, near_gk, near_gv, project_grad)
    summed = jnp.sum(pieces, axis=0)
    matrix = exchange(jnp.broadcast_to(summed[None], (32, 48, 128)), CHIPS)
    matrix_2 = swap(matrix)
    a = jnp.where(core[0] == 0, matrix, matrix_2)
    b = jnp.where(core[0] == 0, matrix_2, matrix)
    return (mixed[None], gr[None], gk[None], gv[None], gx[None],
            a[:, :40].reshape(SPAN // 2, 128), b[:, :40].reshape(SPAN // 2, 128),
            a[:HALF, 40].reshape(SPAN // 2), b[:HALF, 40].reshape(SPAN // 2))


def solution(mesh):
    split = Mesh(mesh.devices.reshape(4, 2, 4, 2, mesh.shape["dp"]), SEQ + ("dp",))
    tokens = P("dp", SEQ, None)
    return jax.shard_map(
        inside,
        mesh=split,
        in_specs=(tokens,) * 5 + (P(),) * 4,
        out_specs=(tokens,) * 5 + (P("dp", None), P("dp", None), P("dp"), P("dp")),
        check_vma=False,
    )
```

```python
import jax
import jax.numpy as jnp
from jax import lax
from jax.experimental import pallas as pl
from jax.experimental.pallas import tpu as pltpu
from jax.sharding import Mesh
from jax.sharding import PartitionSpec as P


LANE_TOTAL = 64
BLOCK = 64
TOKENS = 128
PAIRS = 20
SPAN = 2560
SEQ = ("seq_0", "seq_1", "seq_2", "seq_3")
CHIPS = SEQ[:3]
CORE = SEQ[3]
HALF = 10
HALF_ROWS = 640
CHUNK = 5
STEPS = 4
VMEM_LIMIT = 56
F32 = jnp.float32
BF16 = jnp.bfloat16
NN = (((1,), (0,)), ((), ()))
NT = (((1,), (1,)), ((), ()))
TN = (((0,), (0,)), ((), ()))


def mm(left, right, dims):
    return lax.dot_general(left, right, dims, preferred_element_type=F32)


def iotas():
    rows = lax.broadcasted_iota(jnp.int32, (TOKENS, 128), 0)
    cols = lax.broadcasted_iota(jnp.int32, (TOKENS, 128), 1)
    return rows, cols


def sum_rows(matrix_2, x):
    hi = x.astype(BF16)
    low = (x - hi.astype(F32)).astype(BF16)
    return mm(matrix_2, jnp.concatenate([hi, low], axis=0), NN)


def twice(mask):
    one = mask.astype(F32).astype(BF16)
    return jnp.concatenate([one, one], axis=1)


def apart(x):
    zero = jnp.zeros((BLOCK, x.shape[1]), x.dtype)
    top = jnp.concatenate([x[:BLOCK], zero], axis=1)
    bottom = jnp.concatenate([zero, x[BLOCK:]], axis=1)
    return jnp.concatenate([top, bottom], axis=0)


def per_block(row_of, first):
    top = jnp.broadcast_to(row_of[first : first + 1], (BLOCK, 128))
    bottom = jnp.broadcast_to(row_of[BLOCK + first : BLOCK + first + 1], (BLOCK, 128))
    return jnp.concatenate([top, bottom], axis=0)


def pack(full, low_lanes):
    return jnp.where(low_lanes, full[:LANE_TOTAL], full[LANE_TOTAL:])


def early_kernel(core_ref, x_ref, r_ref, k_ref, v_ref, g_ref, down_ref, up_ref, speed_ref,
                 theirs_ref, mine_ref, smooth_ref, log_ref, inc_ref, reached_ref, faded_ref, own_ref, pull_ref,
                 stage_ref, sems):
    step = pl.program_id(0)
    half = jnp.where(step < 2, 1 - core_ref[0], core_ref[0])

    @pl.when(step == 0)
    def _():
        smooth_ref[...] = jnp.tanh(mm(x_ref[...], down_ref[...], NN))

    gate = smooth_ref[...].astype(BF16)
    rows, cols = iotas()
    lower = twice((rows >= cols) & (rows // BLOCK == cols // BLOCK))
    low_lanes = cols[:LANE_TOTAL] < LANE_TOTAL
    base = (step % 2) * CHUNK
    speed = jnp.concatenate([speed_ref[pl.ds(half * HALF + base + i, 1), :] for i in range(CHUNK)], axis=1)
    log_decays = -speed * jnp.exp(mm(gate, up_ref[...], NT))
    incs = sum_rows(lower, log_decays)
    log_ref[...] = log_decays
    inc_ref[...] = incs
    for i in range(CHUNK):
        lanes = slice(i * 128, i * 128 + 128)
        inc = incs[:, lanes]
        exc = inc - log_decays[:, lanes]
        total = per_block(inc, BLOCK - 1)
        reached = (r_ref[:, lanes].astype(F32) * jnp.exp(exc)).astype(BF16)
        faded = (k_ref[:, lanes].astype(F32) * jnp.exp(total - inc)).astype(BF16)
        reached_ref[:, lanes] = reached
        faded_ref[:, lanes] = faded
        v = v_ref[:, lanes]
        g = g_ref[:, lanes]
        owns = mm(v, apart(faded), TN)
        pulls = mm(g, apart(reached), TN)
        own = [pack(owns[:, b : b + 128], low_lanes) for b in (0, 128)]
        pull = [pack(pulls[:, b : b + 128], low_lanes) for b in (0, 128)]
        total_0 = inc[BLOCK - 1 : BLOCK]
        total_1 = inc[TOKENS - 1 : TOKENS]
        here = slice(i * LANE_TOTAL, i * LANE_TOTAL + LANE_TOTAL)
        own_ref[here, :] = own[0]
        pull_ref[0, here, :] = pull[0]
        pull_ref[1, here, :] = pull[1]
        row = pl.multiple_of((base + i) * LANE_TOTAL, LANE_TOTAL)
        stage_ref[step // 2, pl.ds(row, LANE_TOTAL), :] = jnp.exp(total_1) * own[0] + own[1]
        stage_ref[step // 2, pl.ds(HALF_ROWS + row, LANE_TOTAL), :] = jnp.exp(total_0) * pull[1] + pull[0]
        stage_ref[step // 2, pl.ds(2 * HALF_ROWS + base + i, 1), :] = jnp.exp(total_0 + total_1)

    @pl.when(step == STEPS - 1)
    def _():
        copies = [pltpu.make_async_copy(stage_ref.at[j], ref, sems.at[j]) for j, ref in enumerate((theirs_ref, mine_ref))]
        for copy in copies:
            copy.start()
        for copy in copies:
            copy.wait()


def join_kernel(place_ref, mine_ref, other_ref, send_ref):
    first = place_ref[0] == 0

    def both(rows):
        mine = mine_ref[rows, :]
        other = other_ref[rows, :]
        return jnp.where(first, mine, other), jnp.where(first, other, mine)

    for i in range(HALF):
        decay_a, decay_b = both(slice(2 * HALF_ROWS + i, 2 * HALF_ROWS + i + 1))
        decay = decay_a * decay_b
        for q in range(8):
            at = i * LANE_TOTAL + q * 8
            own_a, own_b = both(slice(at, at + 8))
            pull_a, pull_b = both(slice(HALF_ROWS + at, HALF_ROWS + at + 8))
            for way, state in enumerate((decay_b * own_a + own_b, pull_a + decay_a * pull_b)):
                group = way * 80 + i * 8 + q
                slot, place = divmod(group, 5)
                send_ref[slot, place * 8 : place * 8 + 8, :] = state
                send_ref[slot, 40 + place : 41 + place, :] = decay


def scan_kernel(place_ref, in_ref, out_ref):
    count = in_ref.shape[0]
    flip = place_ref[0]

    def step(e, run):
        at = jnp.where(flip > 0, count - 1 - e, e)
        result = []
        for q in range(5):
            out_ref[at, q * 8 : q * 8 + 8, :] = run[q]
            decay = in_ref[at, 40 + q : 41 + q, :]
            result.append(decay * run[q] + in_ref[at, q * 8 : q * 8 + 8, :])
        return tuple(result)

    lax.fori_loop(0, count, step, tuple(jnp.zeros((8, 128), F32) for _ in range(5)))


def part_kernel(place_ref, chip_ref, mine_ref, other_ref, keep_ref, give_ref):
    first = place_ref[0] == 0

    def both(rows):
        mine = mine_ref[rows, :]
        other = other_ref[rows, :]
        return jnp.where(first, mine, other), jnp.where(first, other, mine)

    for i in range(HALF):
        decay_a, decay_b = both(slice(2 * HALF_ROWS + i, 2 * HALF_ROWS + i + 1))
        ahead = slice(i * LANE_TOTAL, i * LANE_TOTAL + LANE_TOTAL)
        behind = slice(HALF_ROWS + i * LANE_TOTAL, HALF_ROWS + i * LANE_TOTAL + LANE_TOTAL)
        start_a = chip_ref[ahead, :]
        end_b = chip_ref[behind, :]
        start_b = decay_a * start_a + jnp.where(first, mine_ref[ahead, :], other_ref[ahead, :])
        end_a = decay_b * end_b + jnp.where(first, other_ref[behind, :], mine_ref[behind, :])
        keep_ref[ahead, :] = jnp.where(first, start_a, start_b)
        give_ref[ahead, :] = jnp.where(first, start_b, start_a)
        keep_ref[behind, :] = jnp.where(first, end_a, end_b)
        give_ref[behind, :] = jnp.where(first, end_b, end_a)


def two(x, low):
    x = x.astype(F32)
    zero = jnp.zeros_like(x)
    return jnp.concatenate([jnp.where(low, x, zero), jnp.where(low, zero, x)], axis=0).astype(BF16)


def corners(state, low_lanes):
    zero = jnp.zeros_like(state)
    return jnp.concatenate([jnp.where(low_lanes, state, zero), jnp.where(low_lanes, zero, state)], axis=0).astype(BF16)


def beside(x):
    return jnp.concatenate([x[:TOKENS], x[TOKENS:]], axis=1)


def blocks(left, right_0, right_1, dims):
    return mm(apart(left), jnp.concatenate([right_0, right_1], axis=1 if dims == NT else 0), dims)


def near_kernel(core_ref, r_ref, k_ref, v_ref, g_ref, bonus_ref, log_ref, inc_ref,
                fade_ref, mixed_ref, gr_ref, gk_ref, gv_ref, row_ref):
    rows, cols = iotas()
    same = rows // BLOCK == cols // BLOCK
    strict = (rows > cols) & same
    strict_2 = jnp.concatenate([strict, strict], axis=0)
    before = twice(strict)
    heads = ((rows // LANE_TOTAL) == (cols // LANE_TOTAL)).astype(F32).astype(BF16)
    heads_2 = jnp.concatenate([heads, heads], axis=0)
    low = cols < LANE_TOTAL

    def head_sums(x):
        hi = x.astype(BF16)
        rest = (x - hi.astype(F32)).astype(BF16)
        return mm(jnp.concatenate([hi, rest], axis=1), heads_2, NN)

    step = pl.program_id(0)
    parts = []
    for i in range(CHUNK):
        p = step * CHUNK + i
        lanes = slice(i * 128, i * 128 + 128)
        v = v_ref[:, lanes]
        g = g_ref[:, lanes]
        rf = r_ref[:, lanes].astype(F32)
        kf = k_ref[:, lanes].astype(F32)
        vf = v.astype(F32)
        gf = g.astype(F32)
        bonus = bonus_ref[pl.ds(p, 1), :]
        inc = inc_ref[:, lanes]
        exc = inc - log_ref[:, lanes]
        middle = per_block(inc, BLOCK // 2 - 1)
        upward = jnp.exp(exc - middle)
        downward = jnp.exp(middle - inc)
        early = (rf * upward).astype(BF16)
        late = (kf * downward).astype(BF16)
        early_2 = two(early, low)
        late_2 = two(late, low)
        v_2 = two(v, low)
        g_2 = two(g, low)
        scores = jnp.where(strict_2, mm(early_2, late, NT), 0.0).astype(BF16)
        products = jnp.where(strict_2, mm(g_2, v, NT), 0.0).astype(BF16)
        present = head_sums(rf * bonus * kf)
        agree = head_sums(vf * gf)
        mixed_ref[:, lanes] = mm(beside(scores), v_2, NN) + present * vf
        gv_ref[:, lanes] = mm(scores, g_2, TN) + present * gf
        r_near = mm(beside(products), late_2, NN)
        k_near = mm(products, early_2, TN)
        gr_ref[:, lanes] = upward * r_near + bonus * kf * agree
        gk_ref[:, lanes] = downward * k_near + bonus * rf * agree
        row_ref[pl.ds(p, 1), :] = jnp.sum(rf * kf * agree, axis=0, keepdims=True)
        r_part = early.astype(F32) * r_near
        k_part = late.astype(F32) * k_near
        parts.append((r_part, k_part))
    r_parts, k_parts = (jnp.concatenate(z, axis=1) for z in zip(*parts))
    fade_ref[...] = sum_rows(before, k_parts - r_parts) - r_parts


def start_and_end(p, i, core, mine_ref, other_ref, own_ref, pull_ref, decay_0, decay_1):
    half = p // HALF
    row = pl.multiple_of((p - half * HALF) * LANE_TOTAL, LANE_TOTAL)
    here = slice(i * LANE_TOTAL, i * LANE_TOTAL + LANE_TOTAL)

    def of(rows):
        return jnp.where(half == core, mine_ref[rows, :], other_ref[rows, :])

    start_0 = of(pl.ds(row, LANE_TOTAL))
    end_1 = of(pl.ds(HALF_ROWS + row, LANE_TOTAL))
    start_1 = decay_0 * start_0 + own_ref[here, :]
    end_0 = decay_1 * end_1 + pull_ref[1, here, :]
    return start_0, start_1, end_0, end_1


def slope_kernel(core_ref, x_ref, v_ref, g_ref, up_ref, smooth_ref, log_ref, inc_ref, reached_ref, faded_ref, own_ref, pull_ref,
                 mine_ref, other_ref, fade_ref, row_ref, keep_ref, give_ref, project_ref, stage_ref, rest_ref, total_ref, sems):
    core = core_ref[0]
    step = pl.program_id(0)
    smooth = smooth_ref[...]
    gate = smooth.astype(BF16)
    rows, cols = iotas()
    strict = (rows > cols) & (rows // BLOCK == cols // BLOCK)
    before = twice(strict)
    low_lanes = cols[:LANE_TOTAL] < LANE_TOTAL

    def rounded(z):
        return z.astype(BF16).astype(F32)

    spread = range(CHUNK)
    lanes = [slice(i * 128, i * 128 + 128) for i in spread]
    here = [slice(i * LANE_TOTAL, i * LANE_TOTAL + LANE_TOTAL) for i in spread]
    decays = jnp.exp(jnp.concatenate([inc_ref[BLOCK - 1 : BLOCK, :], inc_ref[TOKENS - 1 : TOKENS, :]], axis=0))
    decay = [(decays[0:1, z], decays[1:2, z]) for z in lanes]
    states = [start_and_end(step * CHUNK + i, i, core, mine_ref, other_ref, own_ref, pull_ref, *decay[i]) for i in spread]
    sides = [[corners(z, low_lanes) for z in four] for four in states]
    r_starts = jnp.concatenate([blocks(g_ref[:, lanes[i]], sides[i][0], sides[i][1], NN) for i in spread], axis=1)
    k_ends = jnp.concatenate([blocks(v_ref[:, lanes[i]], sides[i][2], sides[i][3], NN) for i in spread], axis=1)
    couples = []
    for i in spread:
        start_0, start_1, end_0, end_1 = (rounded(z) for z in states[i])
        couple_0 = jnp.sum((decay[i][0] * end_0 + pull_ref[0, here[i], :]) * start_0, axis=0, keepdims=True)
        couple_1 = jnp.sum((decay[i][1] * end_1 + pull_ref[1, here[i], :]) * start_1, axis=0, keepdims=True)
        couples.append(jnp.concatenate([jnp.broadcast_to(couple_0, (BLOCK, 128)), jnp.broadcast_to(couple_1, (BLOCK, 128))], axis=0))
    r_part = reached_ref[...].astype(F32) * r_starts
    k_part = faded_ref[...].astype(F32) * k_ends
    fading = jnp.concatenate(couples, axis=1) + sum_rows(before, k_part - r_part) - r_part + fade_ref[...]
    slope = fading * log_ref[...]
    slope_half = slope.astype(BF16)
    slope_rows = jnp.sum(slope, axis=0, keepdims=True)
    gate_grad = mm(slope_half, up_ref[...], NN)
    tiles = mm(slope_half, gate, TN)
    half = step // 2
    base = (step % 2) * CHUNK
    stage_ref[1 - core, half, pl.ds(pl.multiple_of(base * 128, 128), CHUNK * 128), :] = tiles
    for i in spread:
        rest_ref[core, half, base + i, 0:1, :] = slope_rows[:, lanes[i]]
        rest_ref[1 - core, half, base + i, 0:1, :] = row_ref[pl.ds(step * CHUNK + i, 1), :]

    @pl.when(step == 0)
    def _():
        total_ref[...] = gate_grad

    @pl.when(step > 0)
    def _():
        total_ref[...] += gate_grad

    @pl.when(step == STEPS - 1)
    def _():
        project_grad = (total_ref[...] * (1.0 - smooth * smooth)).astype(BF16)
        project_ref[...] = project_grad

        for c in range(STEPS):
            tiles = mm(x_ref[:, c * CHUNK * 128 : (c + 1) * CHUNK * 128], project_grad, TN)
            stage_ref[core, c // 2, (c % 2) * CHUNK * 128 : (c % 2 + 1) * CHUNK * 128, :] = tiles

        copies = []
        for j, ref in enumerate((keep_ref, give_ref)):
            for half in range(2):
                tiles = stage_ref.at[j, half].reshape(32, 40, 128)
                copies.append(pltpu.make_async_copy(tiles, ref.at[:, half, pl.ds(0, 40), :], sems.at[j, half, 0]))
                copies.append(pltpu.make_async_copy(rest_ref.at[j, half], ref.at[pl.ds(0, HALF), half, pl.ds(40, 8), :], sems.at[j, half, 1]))
        for copy in copies:
            copy.start()
        for copy in copies:
            copy.wait()


def last_kernel(core_ref, v_ref, g_ref, down_ref, log_ref, inc_ref, reached_ref, faded_ref, own_ref, pull_ref, mine_ref, other_ref,
                near_mixed_ref, near_gr_ref, near_gk_ref, near_gv_ref, project_ref,
                mixed_ref, gr_ref, gk_ref, gv_ref, gx_ref):
    _, cols = iotas()
    low_lanes = cols[:LANE_TOTAL] < LANE_TOTAL
    project_grad = project_ref[...]
    core = core_ref[0]
    step = pl.program_id(0)
    for i in range(CHUNK):
        p = step * CHUNK + i
        lanes = slice(i * 128, i * 128 + 128)
        inc = inc_ref[:, lanes]
        decay_0 = jnp.exp(inc[BLOCK - 1 : BLOCK])
        decay_1 = jnp.exp(inc[TOKENS - 1 : TOKENS])
        states = start_and_end(p, i, core, mine_ref, other_ref, own_ref, pull_ref, decay_0, decay_1)
        s_0, s_1, e_0, e_1 = (corners(z, low_lanes) for z in states)
        entering = jnp.exp(inc - log_ref[:, lanes])
        leaving = jnp.exp(per_block(inc, BLOCK - 1) - inc)
        mixed_ref[:, lanes] = (near_mixed_ref[:, lanes] + blocks(reached_ref[:, lanes], s_0, s_1, NT)).astype(BF16)
        gv_ref[:, lanes] = (near_gv_ref[:, lanes] + blocks(faded_ref[:, lanes], e_0, e_1, NT)).astype(BF16)
        gr_ref[:, lanes] = (near_gr_ref[:, lanes] + entering * blocks(g_ref[:, lanes], s_0, s_1, NN)).astype(BF16)
        gk_ref[:, lanes] = (near_gk_ref[:, lanes] + leaving * blocks(v_ref[:, lanes], e_0, e_1, NN)).astype(BF16)
        gx_ref[:, lanes] = mm(project_grad, down_ref[lanes, :], NT).astype(BF16)


def call(kernel, outs, count=0):
    more = {}
    if count:
        more["in_specs"] = [pl.BlockSpec(memory_space=pltpu.SMEM)] + [pl.BlockSpec(memory_space=pltpu.VMEM)] * (count - 1)
    return pl.pallas_call(
        kernel,
        out_shape=[jax.ShapeDtypeStruct(s, d) for s, d in outs],
        compiler_params=pltpu.CompilerParams(vmem_limit_bytes=8 * 1024 * 1024),
        **more,
    )


WIDE = ((TOKENS, SPAN), lambda at: pl.BlockSpec((TOKENS, CHUNK * 128), lambda s, core: (0, at(s, core))))
WEIGHT = ((SPAN, 128), lambda at: pl.BlockSpec((CHUNK * 128, 128), lambda s, core: (at(s, core), 0)))
STATE = ((PAIRS * LANE_TOTAL, 128), lambda at: pl.BlockSpec((CHUNK * LANE_TOTAL, 128), lambda s, core: (at(s, core), 0)))
STATES = ((2, PAIRS * LANE_TOTAL, 128), lambda at: pl.BlockSpec((2, CHUNK * LANE_TOTAL, 128), lambda s, core: (0, at(s, core), 0)))


def whole(*shape):
    return (shape, lambda at: pl.BlockSpec(shape, lambda s, core: (0,) * len(shape)))


def kept(*shape):
    return (shape, lambda at: pl.BlockSpec(memory_space=pl.ANY))


def in_steps(kernel, ins, outs, scratch=(), at=lambda s, core: s, flops=10 ** 9):
    return pl.pallas_call(
        kernel,
        grid_spec=pltpu.PrefetchScalarGridSpec(
            num_scalar_prefetch=1,
            grid=(STEPS,),
            in_specs=[spec(at) for _, spec in ins],
            out_specs=[spec(at) for (_, spec), _ in outs],
            scratch_shapes=list(scratch),
        ),
        out_shape=[jax.ShapeDtypeStruct(shape, dtype) for (shape, _), dtype in outs],
        compiler_params=pltpu.CompilerParams(vmem_limit_bytes=VMEM_LIMIT * 1024 * 1024, dimension_semantics=("arbitrary",)),
        cost_estimate=pl.CostEstimate(flops=flops, bytes_accessed=flops // 1000, transcendentals=0),
    )


def exchange(x, axes):
    return lax.all_to_all(x, axes, 0, 0, tiled=True)


def swap(x):
    return lax.ppermute(x, CORE, [(0, 1), (1, 0)])


ROWS = whole(PAIRS, 128)
SQUARE = whole(TOKENS, 128)
PART_ROWS = 2 * HALF_ROWS + 16
STATE_PART = whole(2 * HALF_ROWS, 128)


def early_call():
    return in_steps(
        early_kernel,
        [whole(TOKENS, SPAN), WIDE, WIDE, WIDE, WIDE, whole(SPAN, 128), WEIGHT, ROWS],
        [(kept(PART_ROWS, 128), F32), (kept(PART_ROWS, 128), F32), (SQUARE, F32), (WIDE, F32), (WIDE, F32), (WIDE, BF16), (WIDE, BF16),
         (STATE, F32), (STATES, F32)],
        (pltpu.VMEM((2, PART_ROWS, 128), F32), pltpu.SemaphoreType.DMA((2,))), lambda s, core: ((1 - core[0]) * 2 + s) % STEPS,
    )


def near_call():
    return in_steps(near_kernel, [WIDE] * 4 + [ROWS, WIDE, WIDE], [(WIDE, F32)] * 5 + [(ROWS, F32)])


def slope_call():
    return in_steps(
        slope_kernel,
        [whole(TOKENS, SPAN), WIDE, WIDE, WEIGHT, SQUARE, WIDE, WIDE, WIDE, WIDE, STATE, STATES, STATE_PART, STATE_PART, WIDE, ROWS],
        [(kept(32, 2, 48, 128), F32), (kept(32, 2, 48, 128), F32), (SQUARE, BF16)],
        (pltpu.VMEM((2, 2, SPAN // 2, 128), F32), pltpu.VMEM((2, 2, HALF, 8, 128), F32), pltpu.VMEM((TOKENS, 128), F32),
         pltpu.SemaphoreType.DMA((2, 2, 2))),
    )


def last_call():
    return in_steps(
        last_kernel,
        [WIDE, WIDE, WEIGHT, WIDE, WIDE, WIDE, WIDE, STATE, STATES, STATE_PART, STATE_PART, WIDE, WIDE, WIDE, WIDE, SQUARE],
        [(WIDE, BF16)] * 5,
    )


def inside(r, k, v, x, g, down, up, speed, bonus):
    r, k, v, x, g = (z[0] for z in (r, k, v, x, g))
    speed = speed.reshape(PAIRS, 128)
    bonus = bonus.reshape(PAIRS, 128)
    core = lax.axis_index(CORE).astype(jnp.int32)[None]
    flip = (lax.axis_index(CHIPS) // 16).astype(jnp.int32)[None]
    theirs, mine, smooth, log_decay, inc, reached, faded, own, pull = early_call()(core, x, r, k, v, g, down, up, speed)
    other = swap(theirs)
    (joined,) = call(join_kernel, [((32, 48, 128), F32)], 3)(core, mine, other)
    there = exchange(joined, CHIPS)
    fade, near_mixed, near_gr, near_gk, near_gv, bonus_rows = near_call()(core, r, k, v, g, bonus, log_decay, inc)
    (scanned,) = call(scan_kernel, [((32, 40, 128), F32)], 2)(flip, there)
    chip = exchange(scanned, CHIPS).reshape(2 * HALF_ROWS, 128)
    keep, give = call(part_kernel, [((2 * HALF_ROWS, 128), F32)] * 2, 4)(core, chip, mine, other)
    got = swap(give)
    held, given, project_grad = slope_call()(core, x, v, g, up, smooth, log_decay, inc, reached, faded, own, pull, keep, got, fade, bonus_rows)
    grads = (held + swap(given)).reshape(64, 48, 128)
    pieces = exchange(grads, CHIPS + ("dp",))
    mixed, gr, gk, gv, gx = last_call()(core, v, g, down, log_decay, inc, reached, faded, own, pull, keep, got, near_mixed, near_gr, near_gk, near_gv, project_grad)
    summed = jnp.sum(pieces, axis=0)
    matrix = exchange(jnp.broadcast_to(summed[None], (32, 48, 128)), CHIPS)
    matrix_2 = swap(matrix)
    a = jnp.where(core[0] == 0, matrix, matrix_2)
    b = jnp.where(core[0] == 0, matrix_2, matrix)
    return (mixed[None], gr[None], gk[None], gv[None], gx[None],
            a[:, :40].reshape(SPAN // 2, 128), b[:, :40].reshape(SPAN // 2, 128),
            a[:HALF, 40].reshape(SPAN // 2), b[:HALF, 40].reshape(SPAN // 2))


def solution(mesh):
    split = Mesh(mesh.devices.reshape(4, 2, 4, 2, mesh.shape["dp"]), SEQ + ("dp",))
    tokens = P("dp", SEQ, None)
    return jax.shard_map(
        inside,
        mesh=split,
        in_specs=(tokens,) * 5 + (P(),) * 4,
        out_specs=(tokens,) * 5 + (P("dp", None), P("dp", None), P("dp"), P("dp")),
        check_vma=False,
    )
```

```python
import jax
import jax.numpy as jnp
from jax import lax
from jax.experimental import pallas as pl
from jax.experimental.pallas import tpu as pltpu
from jax.sharding import Mesh
from jax.sharding import PartitionSpec as P


LANE_TOTAL = 64
BLOCK = 64
TOKENS = 128
PAIRS = 20
SPAN = 2560
SEQ = ("seq_0", "seq_1", "seq_2", "seq_3")
CHIPS = SEQ[:3]
CORE = SEQ[3]
HALF = 10
HALF_ROWS = 640
CHUNK = 5
STEPS = 4
VMEM_LIMIT = 24
FREE = ((32, 2, 48, 128), (1296, 128))
F32 = jnp.float32
BF16 = jnp.bfloat16
NN = (((1,), (0,)), ((), ()))
NT = (((1,), (1,)), ((), ()))
TN = (((0,), (0,)), ((), ()))


def mm(left, right, dims):
    return lax.dot_general(left, right, dims, preferred_element_type=F32)


def iotas():
    rows = lax.broadcasted_iota(jnp.int32, (TOKENS, 128), 0)
    cols = lax.broadcasted_iota(jnp.int32, (TOKENS, 128), 1)
    return rows, cols


def sum_rows(matrix_2, x):
    hi = x.astype(BF16)
    low = (x - hi.astype(F32)).astype(BF16)
    return mm(matrix_2, jnp.concatenate([hi, low], axis=0), NN)


def twice(mask):
    one = mask.astype(F32).astype(BF16)
    return jnp.concatenate([one, one], axis=1)


def apart(x):
    zero = jnp.zeros((BLOCK, x.shape[1]), x.dtype)
    top = jnp.concatenate([x[:BLOCK], zero], axis=1)
    bottom = jnp.concatenate([zero, x[BLOCK:]], axis=1)
    return jnp.concatenate([top, bottom], axis=0)


def per_block(row_of, first):
    top = jnp.broadcast_to(row_of[first : first + 1], (BLOCK, 128))
    bottom = jnp.broadcast_to(row_of[BLOCK + first : BLOCK + first + 1], (BLOCK, 128))
    return jnp.concatenate([top, bottom], axis=0)


def pack(full, low_lanes):
    return jnp.where(low_lanes, full[:LANE_TOTAL], full[LANE_TOTAL:])


def early_steps(half, gate, r_ref, k_ref, v_ref, g_ref, up_ref, speed_ref,
                log_ref, reached_ref, faded_ref, own_ref, pull_ref, total_ref, send_ref):
    step = pl.program_id(0)
    lower = lower_twice()
    low_lanes = iotas()[1][:LANE_TOTAL] < LANE_TOTAL
    base = step * CHUNK
    speed = jnp.concatenate([speed_ref[pl.ds(half * HALF + base + i, 1), :] for i in range(CHUNK)], axis=1)
    log_decays = -speed * jnp.exp(mm(gate, up_ref[...], NT))
    incs = sum_rows(lower, log_decays)
    log_ref[...] = log_decays
    for i in range(CHUNK):
        lanes = slice(i * 128, i * 128 + 128)
        inc = incs[:, lanes]
        exc = inc - log_decays[:, lanes]
        total = per_block(inc, BLOCK - 1)
        reached = (r_ref[:, lanes].astype(F32) * jnp.exp(exc)).astype(BF16)
        faded = (k_ref[:, lanes].astype(F32) * jnp.exp(total - inc)).astype(BF16)
        reached_ref[:, lanes] = reached
        faded_ref[:, lanes] = faded
        owns = mm(v_ref[:, lanes], apart(faded), TN)
        pulls = mm(g_ref[:, lanes], apart(reached), TN)
        own = [pack(owns[:, b : b + 128], low_lanes) for b in (0, 128)]
        pull = [pack(pulls[:, b : b + 128], low_lanes) for b in (0, 128)]
        total_0 = inc[BLOCK - 1 : BLOCK]
        total_1 = inc[TOKENS - 1 : TOKENS]
        here = slice(i * LANE_TOTAL, i * LANE_TOTAL + LANE_TOTAL)
        own_ref[here, :] = own[0]
        pull_ref[0, here, :] = pull[0]
        pull_ref[1, here, :] = pull[1]
        total_ref[0, 0:1, lanes] = total_0
        total_ref[0, 1:2, lanes] = total_1
        row = pl.multiple_of((base + i) * LANE_TOTAL, LANE_TOTAL)
        send_ref[pl.ds(row, LANE_TOTAL), :] = jnp.exp(total_1) * own[0] + own[1]
        send_ref[pl.ds(HALF_ROWS + row, LANE_TOTAL), :] = jnp.exp(total_0) * pull[1] + pull[0]
        send_ref[pl.ds(2 * HALF_ROWS + base + i, 1), :] = jnp.exp(total_0 + total_1)


def lower_twice():
    rows, cols = iotas()
    return twice((rows >= cols) & (rows // BLOCK == cols // BLOCK))


def theirs_kernel(core_ref, x_ref, down_ref, r_ref, k_ref, v_ref, g_ref, up_ref, speed_ref, smooth_ref, *outs):
    @pl.when(pl.program_id(0) == 0)
    def _():
        smooth_ref[...] = jnp.tanh(mm(x_ref[...], down_ref[...], NN))

    early_steps(1 - core_ref[0], smooth_ref[...].astype(BF16), r_ref, k_ref, v_ref, g_ref, up_ref, speed_ref, *outs)


def mine_kernel(core_ref, smooth_ref, r_ref, k_ref, v_ref, g_ref, up_ref, speed_ref, *rest):
    early_steps(core_ref[0], smooth_ref[...].astype(BF16), r_ref, k_ref, v_ref, g_ref, up_ref, speed_ref, *rest[6:])


def join_kernel(place_ref, mine_ref, other_ref, send_ref):
    first = place_ref[0] == 0

    def both(rows):
        mine = mine_ref[rows, :]
        other = other_ref[rows, :]
        return jnp.where(first, mine, other), jnp.where(first, other, mine)

    for i in range(HALF):
        decay_a, decay_b = both(slice(2 * HALF_ROWS + i, 2 * HALF_ROWS + i + 1))
        decay = decay_a * decay_b
        for q in range(8):
            at = i * LANE_TOTAL + q * 8
            own_a, own_b = both(slice(at, at + 8))
            pull_a, pull_b = both(slice(HALF_ROWS + at, HALF_ROWS + at + 8))
            for way, state in enumerate((decay_b * own_a + own_b, pull_a + decay_a * pull_b)):
                group = way * 80 + i * 8 + q
                slot, place = divmod(group, 5)
                send_ref[slot, place * 8 : place * 8 + 8, :] = state
                send_ref[slot, 40 + place : 41 + place, :] = decay


def scan_kernel(place_ref, in_ref, out_ref):
    count = in_ref.shape[0]
    flip = place_ref[0]

    def step(e, run):
        at = jnp.where(flip > 0, count - 1 - e, e)
        result = []
        for q in range(5):
            out_ref[at, q * 8 : q * 8 + 8, :] = run[q]
            decay = in_ref[at, 40 + q : 41 + q, :]
            result.append(decay * run[q] + in_ref[at, q * 8 : q * 8 + 8, :])
        return tuple(result)

    lax.fori_loop(0, count, step, tuple(jnp.zeros((8, 128), F32) for _ in range(5)))


def part_kernel(place_ref, chip_ref, mine_ref, other_ref, keep_ref, give_ref):
    first = place_ref[0] == 0

    def both(rows):
        mine = mine_ref[rows, :]
        other = other_ref[rows, :]
        return jnp.where(first, mine, other), jnp.where(first, other, mine)

    for i in range(HALF):
        decay_a, decay_b = both(slice(2 * HALF_ROWS + i, 2 * HALF_ROWS + i + 1))
        ahead = slice(i * LANE_TOTAL, i * LANE_TOTAL + LANE_TOTAL)
        behind = slice(HALF_ROWS + i * LANE_TOTAL, HALF_ROWS + i * LANE_TOTAL + LANE_TOTAL)
        start_a = chip_ref[ahead, :]
        end_b = chip_ref[behind, :]
        start_b = decay_a * start_a + jnp.where(first, mine_ref[ahead, :], other_ref[ahead, :])
        end_a = decay_b * end_b + jnp.where(first, other_ref[behind, :], mine_ref[behind, :])
        keep_ref[ahead, :] = jnp.where(first, start_a, start_b)
        give_ref[ahead, :] = jnp.where(first, start_b, start_a)
        keep_ref[behind, :] = jnp.where(first, end_a, end_b)
        give_ref[behind, :] = jnp.where(first, end_b, end_a)


def two(x, low):
    x = x.astype(F32)
    zero = jnp.zeros_like(x)
    return jnp.concatenate([jnp.where(low, x, zero), jnp.where(low, zero, x)], axis=0).astype(BF16)


def corners(state, low_lanes):
    zero = jnp.zeros_like(state)
    return jnp.concatenate([jnp.where(low_lanes, state, zero), jnp.where(low_lanes, zero, state)], axis=0).astype(BF16)


def beside(x):
    return jnp.concatenate([x[:TOKENS], x[TOKENS:]], axis=1)


def blocks(left, right_0, right_1, dims):
    return mm(apart(left), jnp.concatenate([right_0, right_1], axis=1 if dims == NT else 0), dims)


def near_kernel(core_ref, r_ref, k_ref, v_ref, g_ref, bonus_ref, log_ref,
                fade_ref, mixed_ref, gr_ref, gk_ref, gv_ref, row_ref):
    rows, cols = iotas()
    same = rows // BLOCK == cols // BLOCK
    strict = (rows > cols) & same
    strict_2 = jnp.concatenate([strict, strict], axis=0)
    before = twice(strict)
    heads = ((rows // LANE_TOTAL) == (cols // LANE_TOTAL)).astype(F32).astype(BF16)
    heads_2 = jnp.concatenate([heads, heads], axis=0)
    low = cols < LANE_TOTAL

    def head_sums(x):
        hi = x.astype(BF16)
        rest = (x - hi.astype(F32)).astype(BF16)
        return mm(jnp.concatenate([hi, rest], axis=1), heads_2, NN)

    step = pl.program_id(0)
    parts = []
    incs = sum_rows(lower_twice(), log_ref[...])
    for i in range(CHUNK):
        p = step * CHUNK + i
        lanes = slice(i * 128, i * 128 + 128)
        v = v_ref[:, lanes]
        g = g_ref[:, lanes]
        rf = r_ref[:, lanes].astype(F32)
        kf = k_ref[:, lanes].astype(F32)
        vf = v.astype(F32)
        gf = g.astype(F32)
        bonus = bonus_ref[pl.ds(p, 1), :]
        inc = incs[:, lanes]
        exc = inc - log_ref[:, lanes]
        middle = per_block(inc, BLOCK // 2 - 1)
        upward = jnp.exp(exc - middle)
        downward = jnp.exp(middle - inc)
        early = (rf * upward).astype(BF16)
        late = (kf * downward).astype(BF16)
        early_2 = two(early, low)
        late_2 = two(late, low)
        v_2 = two(v, low)
        g_2 = two(g, low)
        scores = jnp.where(strict_2, mm(early_2, late, NT), 0.0).astype(BF16)
        products = jnp.where(strict_2, mm(g_2, v, NT), 0.0).astype(BF16)
        present = head_sums(rf * bonus * kf)
        agree = head_sums(vf * gf)
        mixed_ref[:, lanes] = mm(beside(scores), v_2, NN) + present * vf
        gv_ref[:, lanes] = mm(scores, g_2, TN) + present * gf
        r_near = mm(beside(products), late_2, NN)
        k_near = mm(products, early_2, TN)
        gr_ref[:, lanes] = upward * r_near + bonus * kf * agree
        gk_ref[:, lanes] = downward * k_near + bonus * rf * agree
        row_ref[pl.ds(p, 1), :] = jnp.sum(rf * kf * agree, axis=0, keepdims=True)
        r_part = early.astype(F32) * r_near
        k_part = late.astype(F32) * k_near
        parts.append((r_part, k_part))
    r_parts, k_parts = (jnp.concatenate(z, axis=1) for z in zip(*parts))
    fade_ref[...] = sum_rows(before, k_parts - r_parts) - r_parts


def start_and_end(i, start_0, end_1, own_ref, pull_ref, decay_0, decay_1):
    here = slice(i * LANE_TOTAL, i * LANE_TOTAL + LANE_TOTAL)
    start_1 = decay_0 * start_0 + own_ref[here, :]
    end_0 = decay_1 * end_1 + pull_ref[1, here, :]
    return start_0, start_1, end_0, end_1


def slope_steps(v_ref, g_ref, log_ref, total_ref, reached_ref, faded_ref, own_ref, pull_ref, state_ref, fade_ref):
    step = pl.program_id(0)
    rows, cols = iotas()
    before = twice((rows > cols) & (rows // BLOCK == cols // BLOCK))
    low_lanes = cols[:LANE_TOTAL] < LANE_TOTAL

    def rounded(z):
        return z.astype(BF16).astype(F32)

    spread = range(CHUNK)
    lanes = [slice(i * 128, i * 128 + 128) for i in spread]
    here = [slice(i * LANE_TOTAL, i * LANE_TOTAL + LANE_TOTAL) for i in spread]
    decays = jnp.exp(total_ref[0, 0:2, :])
    decay = [(decays[0:1, z], decays[1:2, z]) for z in lanes]
    states = []
    for i in spread:
        row = pl.multiple_of((step * CHUNK + i) * LANE_TOTAL, LANE_TOTAL)
        pair = state_ref[pl.ds(row, LANE_TOTAL), :], state_ref[pl.ds(HALF_ROWS + row, LANE_TOTAL), :]
        states.append(start_and_end(i, *pair, own_ref, pull_ref, *decay[i]))
    sides = [[corners(z, low_lanes) for z in four] for four in states]
    r_starts = jnp.concatenate([blocks(g_ref[:, lanes[i]], sides[i][0], sides[i][1], NN) for i in spread], axis=1)
    k_ends = jnp.concatenate([blocks(v_ref[:, lanes[i]], sides[i][2], sides[i][3], NN) for i in spread], axis=1)
    couples = []
    for i in spread:
        start_0, start_1, end_0, end_1 = (rounded(z) for z in states[i])
        couple_0 = jnp.sum((decay[i][0] * end_0 + pull_ref[0, here[i], :]) * start_0, axis=0, keepdims=True)
        couple_1 = jnp.sum((decay[i][1] * end_1 + pull_ref[1, here[i], :]) * start_1, axis=0, keepdims=True)
        couples.append(jnp.concatenate([jnp.broadcast_to(couple_0, (BLOCK, 128)), jnp.broadcast_to(couple_1, (BLOCK, 128))], axis=0))
    r_part = reached_ref[...].astype(F32) * r_starts
    k_part = faded_ref[...].astype(F32) * k_ends
    fading = jnp.concatenate(couples, axis=1) + sum_rows(before, k_part - r_part) - r_part + fade_ref[...]
    slope = fading * log_ref[...]
    return slope.astype(BF16), jnp.sum(slope, axis=0, keepdims=True)


def slope_kernel(core_ref, v_ref, g_ref, log_ref, total_ref, reached_ref, faded_ref, own_ref, pull_ref, state_ref, fade_ref,
                 slope_ref, sums_ref):
    slope_half, sums = slope_steps(v_ref, g_ref, log_ref, total_ref, reached_ref, faded_ref, own_ref, pull_ref, state_ref, fade_ref)
    slope_ref[...] = slope_half
    for i in range(CHUNK):
        sums_ref[pl.ds(pl.program_id(0) * CHUNK + i, 1), :] = sums[:, i * 128 : i * 128 + 128]


def grads_kernel(core_ref, v_ref, g_ref, log_ref, total_ref, reached_ref, faded_ref, own_ref, pull_ref, state_ref, fade_ref,
                 x_ref, up_ref, smooth_ref, slope_ref, sums_ref, row_ref,
                 keep_ref, give_ref, project_ref, stage_ref, rest_ref, gate_ref, sems):
    core = core_ref[0]
    step = pl.program_id(0)
    smooth = smooth_ref[...]
    gate = smooth.astype(BF16)
    width = CHUNK * 128

    def rows_of(half, at):
        return pl.ds(pl.multiple_of(half * (SPAN // 2) + at * width, 128), width)

    @pl.when(step == 0)
    def _():
        slopes = slope_ref[...]
        stage_ref[1 - core, core] = mm(slopes, gate, TN)
        gate_ref[...] = mm(slopes, up_ref[pl.ds(pl.multiple_of(core * (SPAN // 2), 128), SPAN // 2), :], NN)
        for i in range(HALF):
            rest_ref[core, core, i, 0:1, :] = sums_ref[i : i + 1, :]
            for half in range(2):
                rest_ref[1 - core, half, i, 0:1, :] = row_ref[half * HALF + i : half * HALF + i + 1, :]

    slope_half, sums = slope_steps(v_ref, g_ref, log_ref, total_ref, reached_ref, faded_ref, own_ref, pull_ref, state_ref, fade_ref)
    stage_ref[1 - core, 1 - core, pl.ds(pl.multiple_of(step * width, 128), width), :] = mm(slope_half, gate, TN)
    for i in range(CHUNK):
        rest_ref[core, 1 - core, step * CHUNK + i, 0:1, :] = sums[:, i * 128 : i * 128 + 128]
    gate_ref[...] += mm(slope_half, up_ref[rows_of(1 - core, step), :], NN)

    @pl.when(step == 1)
    def _():
        project_grad = (gate_ref[...] * (1.0 - smooth * smooth)).astype(BF16)
        project_ref[...] = project_grad
        for c in range(4):
            stage_ref[core, c // 2, c % 2 * width : (c % 2 + 1) * width, :] = mm(x_ref[:, c * width : (c + 1) * width], project_grad, TN)
        copies = []
        for j, ref in enumerate((keep_ref, give_ref)):
            for half in range(2):
                tiles = stage_ref.at[j, half].reshape(32, 40, 128)
                copies.append(pltpu.make_async_copy(tiles, ref.at[:, half, pl.ds(0, 40), :], sems.at[j, half, 0]))
                copies.append(pltpu.make_async_copy(rest_ref.at[j, half], ref.at[pl.ds(0, HALF), half, pl.ds(40, 8), :], sems.at[j, half, 1]))
        for copy in copies:
            copy.start()
        for copy in copies:
            copy.wait()


def last_kernel(core_ref, v_ref, g_ref, down_ref, log_ref, reached_ref, faded_ref, own_ref, pull_ref, mine_ref, other_ref,
                near_mixed_ref, near_gr_ref, near_gk_ref, near_gv_ref, project_ref,
                mixed_ref, gr_ref, gk_ref, gv_ref, gx_ref):
    _, cols = iotas()
    low_lanes = cols[:LANE_TOTAL] < LANE_TOTAL
    project_grad = project_ref[...]
    core = core_ref[0]
    step = pl.program_id(0)
    incs = sum_rows(lower_twice(), log_ref[...])
    for i in range(CHUNK):
        lanes = slice(i * 128, i * 128 + 128)
        inc = incs[:, lanes]
        decay_0 = jnp.exp(inc[BLOCK - 1 : BLOCK])
        decay_1 = jnp.exp(inc[TOKENS - 1 : TOKENS])
        row = pl.multiple_of((step % 2 * CHUNK + i) * LANE_TOTAL, LANE_TOTAL)
        pair = [jnp.where(step // 2 == core, mine_ref[at, :], other_ref[at, :])
                for at in (pl.ds(row, LANE_TOTAL), pl.ds(HALF_ROWS + row, LANE_TOTAL))]
        states = start_and_end(i, *pair, own_ref, pull_ref, decay_0, decay_1)
        s_0, s_1, e_0, e_1 = (corners(z, low_lanes) for z in states)
        entering = jnp.exp(inc - log_ref[:, lanes])
        leaving = jnp.exp(per_block(inc, BLOCK - 1) - inc)
        mixed_ref[:, lanes] = (near_mixed_ref[:, lanes] + blocks(reached_ref[:, lanes], s_0, s_1, NT)).astype(BF16)
        gv_ref[:, lanes] = (near_gv_ref[:, lanes] + blocks(faded_ref[:, lanes], e_0, e_1, NT)).astype(BF16)
        gr_ref[:, lanes] = (near_gr_ref[:, lanes] + entering * blocks(g_ref[:, lanes], s_0, s_1, NN)).astype(BF16)
        gk_ref[:, lanes] = (near_gk_ref[:, lanes] + leaving * blocks(v_ref[:, lanes], e_0, e_1, NN)).astype(BF16)
        gx_ref[:, lanes] = mm(project_grad, down_ref[lanes, :], NT).astype(BF16)


def final_kernel(core_ref, mine_ref, other_ref, a_ref, b_ref, a_row_ref, b_row_ref, sems):
    first = core_ref[0] == 0

    def send(x_ref, y_ref):
        copies = [pltpu.make_async_copy(z.at[:, pl.ds(0, 40), :], ref, sems.at[j]) for j, (z, ref) in enumerate(((x_ref, a_ref), (y_ref, b_ref)))]
        for copy in copies:
            copy.start()
        for i in range(HALF):
            a_row_ref[i : i + 1, :] = x_ref[i, 40:41, :]
            b_row_ref[i : i + 1, :] = y_ref[i, 40:41, :]
        for copy in copies:
            copy.wait()

    pl.when(first)(lambda: send(mine_ref, other_ref))
    pl.when(jnp.logical_not(first))(lambda: send(other_ref, mine_ref))


def final_call():
    vmem = pl.BlockSpec(memory_space=pltpu.VMEM)
    hbm = pl.BlockSpec(memory_space=pl.ANY)
    return pl.pallas_call(
        final_kernel,
        in_specs=[pl.BlockSpec(memory_space=pltpu.SMEM), vmem, vmem],
        out_specs=[hbm, hbm, vmem, vmem],
        out_shape=[jax.ShapeDtypeStruct(z, F32) for z in ((32, 40, 128), (32, 40, 128), (HALF, 128), (HALF, 128))],
        scratch_shapes=[pltpu.SemaphoreType.DMA((2,))],
        compiler_params=pltpu.CompilerParams(vmem_limit_bytes=8 * 1024 * 1024),
        name="final",
    )


def call(kernel, outs, count=0):
    more = {}
    if count:
        more["in_specs"] = [pl.BlockSpec(memory_space=pltpu.SMEM)] + [pl.BlockSpec(memory_space=pltpu.VMEM)] * (count - 1)
    return pl.pallas_call(
        kernel,
        out_shape=[jax.ShapeDtypeStruct(s, d) for s, d in outs],
        compiler_params=pltpu.CompilerParams(vmem_limit_bytes=8 * 1024 * 1024),
        **more,
    )


WIDE = ((TOKENS, SPAN), lambda at: pl.BlockSpec((TOKENS, CHUNK * 128), lambda s, core: (0, at(s, core))))
WEIGHT = ((SPAN, 128), lambda at: pl.BlockSpec((CHUNK * 128, 128), lambda s, core: (at(s, core), 0)))
STATE = ((PAIRS * LANE_TOTAL, 128), lambda at: pl.BlockSpec((CHUNK * LANE_TOTAL, 128), lambda s, core: (at(s, core), 0)))
STATES = ((2, PAIRS * LANE_TOTAL, 128), lambda at: pl.BlockSpec((2, CHUNK * LANE_TOTAL, 128), lambda s, core: (0, at(s, core), 0)))


def whole(*shape):
    return (shape, lambda at: pl.BlockSpec(shape, lambda s, core: (0,) * len(shape)))


def kept(*shape):
    return (shape, lambda at: pl.BlockSpec(memory_space=pl.ANY))


TOTAL = ((STEPS, 2, CHUNK * 128), lambda at: pl.BlockSpec((1, 2, CHUNK * 128), lambda s, core: (at(s, core), 0, 0)))


def in_steps(kernel, ins, outs, scratch=(), at=lambda s, core: s, steps=STEPS, aliases=None, flops=10 ** 9):
    return pl.pallas_call(
        kernel,
        grid_spec=pltpu.PrefetchScalarGridSpec(
            num_scalar_prefetch=1,
            grid=(steps,),
            in_specs=[spec(at) for _, spec in ins],
            out_specs=[spec(at) for (_, spec), _ in outs],
            scratch_shapes=list(scratch),
        ),
        out_shape=[jax.ShapeDtypeStruct(shape, dtype) if shape in FREE else pltpu.HBM(shape, dtype) for (shape, spec), dtype in outs],
        compiler_params=pltpu.CompilerParams(vmem_limit_bytes=VMEM_LIMIT * 1024 * 1024, dimension_semantics=("arbitrary",)),
        cost_estimate=pl.CostEstimate(flops=flops, bytes_accessed=flops // 1000, transcendentals=0),
        input_output_aliases=aliases or {},
    )


ROWS = whole(PAIRS, 128)
SQUARE = whole(TOKENS, 128)
PART = whole(2 * HALF_ROWS + 16, 128)
STATE_PART = whole(2 * HALF_ROWS, 128)
HALF_WIDE = ((TOKENS, SPAN // 2), lambda at: pl.BlockSpec((TOKENS, CHUNK * 128), lambda s, core: (0, s)))
EARLY = [(WIDE, F32), (WIDE, BF16), (WIDE, BF16), (STATE, F32), (STATES, F32), (TOTAL, F32)]
SLOPE = [WIDE, WIDE, WIDE, TOTAL, WIDE, WIDE, STATE, STATES, STATE_PART, WIDE]


def mine_half(s, core):
    return core[0] * 2 + s


def their_half(s, core):
    return (1 - core[0]) * 2 + s


def theirs_call():
    return in_steps(
        theirs_kernel, [whole(TOKENS, SPAN), whole(SPAN, 128), WIDE, WIDE, WIDE, WIDE, WEIGHT, ROWS],
        [(SQUARE, F32)] + EARLY + [(PART, F32)], at=their_half, steps=2,
    )


def mine_call():
    return in_steps(
        mine_kernel, [SQUARE, WIDE, WIDE, WIDE, WIDE, WEIGHT, ROWS] + [kept(*z[0][0]) for z in EARLY],
        EARLY + [(PART, F32)], at=mine_half, steps=2, aliases={8 + j: j for j in range(len(EARLY))},
    )


def near_call():
    return in_steps(near_kernel, [WIDE] * 4 + [ROWS, WIDE], [(WIDE, F32)] * 5 + [(ROWS, F32)])


def slope_call():
    return in_steps(slope_kernel, SLOPE, [(HALF_WIDE, BF16), (whole(HALF, 128), F32)], at=mine_half, steps=2)


def grads_call():
    return in_steps(
        grads_kernel, SLOPE + [whole(TOKENS, SPAN), whole(SPAN, 128), SQUARE, whole(TOKENS, SPAN // 2), whole(HALF, 128), ROWS],
        [(kept(32, 2, 48, 128), F32), (kept(32, 2, 48, 128), F32), (SQUARE, BF16)],
        (pltpu.VMEM((2, 2, SPAN // 2, 128), F32), pltpu.VMEM((2, 2, HALF, 8, 128), F32), pltpu.VMEM((TOKENS, 128), F32),
         pltpu.SemaphoreType.DMA((2, 2, 2))),
        at=their_half, steps=2,
    )


def last_call():
    return in_steps(
        last_kernel,
        [WIDE, WIDE, WEIGHT, WIDE, WIDE, WIDE, STATE, STATES, STATE_PART, STATE_PART, WIDE, WIDE, WIDE, WIDE, SQUARE],
        [(WIDE, BF16)] * 5,
    )


def exchange(x, axes):
    return lax.all_to_all(x, axes, 0, 0, tiled=True)


def swap(x):
    return lax.ppermute(x, CORE, [(0, 1), (1, 0)])


def far(*arrays):
    return [pltpu.with_memory_space_constraint(z, pltpu.HBM) for z in arrays]


def inside(r, k, v, x, g, down, up, speed, bonus):
    r, k, v, x, g = (z[0] for z in (r, k, v, x, g))
    speed = speed.reshape(PAIRS, 128)
    bonus = bonus.reshape(PAIRS, 128)
    r, k, v, x, g, down, up, speed, bonus = far(r, k, v, x, g, down, up, speed, bonus)
    core = lax.axis_index(CORE).astype(jnp.int32)[None]
    flip = (lax.axis_index(CHIPS) // 16).astype(jnp.int32)[None]
    smooth, *early, theirs = theirs_call()(core, x, down, r, k, v, g, up, speed)
    (smooth,) = far(smooth)
    other = swap(theirs)
    *early, mine = mine_call()(core, smooth, r, k, v, g, up, speed, *far(*early))
    log_decay, reached, faded, own, pull, total = far(*early)
    (joined,) = call(join_kernel, [((32, 48, 128), F32)], 3)(core, mine, other)
    there = exchange(joined, CHIPS)
    near = near_call()(core, r, k, v, g, bonus, log_decay)
    fade, near_mixed, near_gr, near_gk, near_gv, bonus_rows = far(*near)
    (scanned,) = call(scan_kernel, [((32, 40, 128), F32)], 2)(flip, there)
    chip = exchange(scanned, CHIPS).reshape(2 * HALF_ROWS, 128)
    keep, give = call(part_kernel, [((2 * HALF_ROWS, 128), F32)] * 2, 4)(core, chip, mine, other)
    got = swap(give)
    slope_mine, sums_mine = far(*slope_call()(core, v, g, log_decay, total, reached, faded, own, pull, keep, fade))
    held, given, project_grad = grads_call()(core, v, g, log_decay, total, reached, faded, own, pull, got, fade,
                                             x, up, smooth, slope_mine, sums_mine, bonus_rows)
    (project_grad,) = far(project_grad)
    grads = (held + swap(given)).reshape(64, 48, 128)
    pieces = exchange(grads, CHIPS + ("dp",))
    mixed, gr, gk, gv, gx = last_call()(core, v, g, down, log_decay, reached, faded, own, pull, keep, got,
                                        near_mixed, near_gr, near_gk, near_gv, project_grad)
    summed = jnp.sum(pieces, axis=0)
    matrix = exchange(jnp.broadcast_to(summed[None], (32, 48, 128)), CHIPS)
    a, b, a_row, b_row = final_call()(core, matrix, swap(matrix))
    return (mixed[None], gr[None], gk[None], gv[None], gx[None],
            a.reshape(SPAN // 2, 128), b.reshape(SPAN // 2, 128), a_row.reshape(SPAN // 2), b_row.reshape(SPAN // 2))


def solution(mesh):
    split = Mesh(mesh.devices.reshape(4, 2, 4, 2, mesh.shape["dp"]), SEQ + ("dp",))
    tokens = P("dp", SEQ, None)
    return jax.shard_map(
        inside,
        mesh=split,
        in_specs=(tokens,) * 5 + (P(),) * 4,
        out_specs=(tokens,) * 5 + (P("dp", None), P("dp", None), P("dp"), P("dp")),
        check_vma=False,
    )
```

```python
import jax
import jax.numpy as jnp
from jax import lax
from jax.experimental import pallas as pl
from jax.experimental.pallas import tpu as pltpu
from jax.sharding import Mesh
from jax.sharding import PartitionSpec as P


LANE_TOTAL = 64
BLOCK = 64
TOKENS = 128
PAIRS = 20
SPAN = 2560
SEQ = ("seq_0", "seq_1", "seq_2", "seq_3")
CHIPS = SEQ[:3]
CORE = SEQ[3]
HALF = 10
HALF_ROWS = 640
CHUNK = 10
HALF_STEPS = HALF // CHUNK
STEPS = 2 * HALF_STEPS
VMEM_LIMIT = 24
FREE = ((32, 2, 48, 128), (1296, 128))
F32 = jnp.float32
BF16 = jnp.bfloat16
NN = (((1,), (0,)), ((), ()))
NT = (((1,), (1,)), ((), ()))
TN = (((0,), (0,)), ((), ()))


def mm(left, right, dims):
    return lax.dot_general(left, right, dims, preferred_element_type=F32)


def iotas():
    rows = lax.broadcasted_iota(jnp.int32, (TOKENS, 128), 0)
    cols = lax.broadcasted_iota(jnp.int32, (TOKENS, 128), 1)
    return rows, cols


def sum_rows(matrix_2, x):
    hi = x.astype(BF16)
    low = (x - hi.astype(F32)).astype(BF16)
    return mm(matrix_2, jnp.concatenate([hi, low], axis=0), NN)


def twice(mask):
    one = mask.astype(F32).astype(BF16)
    return jnp.concatenate([one, one], axis=1)


def apart(x):
    zero = jnp.zeros((BLOCK, x.shape[1]), x.dtype)
    top = jnp.concatenate([x[:BLOCK], zero], axis=1)
    bottom = jnp.concatenate([zero, x[BLOCK:]], axis=1)
    return jnp.concatenate([top, bottom], axis=0)


def per_block(row_of, first):
    top = jnp.broadcast_to(row_of[first : first + 1], (BLOCK, 128))
    bottom = jnp.broadcast_to(row_of[BLOCK + first : BLOCK + first + 1], (BLOCK, 128))
    return jnp.concatenate([top, bottom], axis=0)


def pack(full, low_lanes):
    return jnp.where(low_lanes, full[:LANE_TOTAL], full[LANE_TOTAL:])


def early_steps(half, gate, r_ref, k_ref, v_ref, g_ref, up_ref, speed_ref,
                log_ref, reached_ref, faded_ref, own_ref, pull_ref, total_ref, send_ref):
    step = pl.program_id(0)
    lower = lower_twice()
    low_lanes = iotas()[1][:LANE_TOTAL] < LANE_TOTAL
    base = step * CHUNK
    speed = jnp.concatenate([speed_ref[pl.ds(half * HALF + base + i, 1), :] for i in range(CHUNK)], axis=1)
    log_decays = -speed * jnp.exp(mm(gate, up_ref[...], NT))
    incs = sum_rows(lower, log_decays)
    log_ref[...] = log_decays
    for i in range(CHUNK):
        lanes = slice(i * 128, i * 128 + 128)
        inc = incs[:, lanes]
        exc = inc - log_decays[:, lanes]
        total = per_block(inc, BLOCK - 1)
        reached = (r_ref[:, lanes].astype(F32) * jnp.exp(exc)).astype(BF16)
        faded = (k_ref[:, lanes].astype(F32) * jnp.exp(total - inc)).astype(BF16)
        reached_ref[:, lanes] = reached
        faded_ref[:, lanes] = faded
        owns = mm(v_ref[:, lanes], apart(faded), TN)
        pulls = mm(g_ref[:, lanes], apart(reached), TN)
        own = [pack(owns[:, b : b + 128], low_lanes) for b in (0, 128)]
        pull = [pack(pulls[:, b : b + 128], low_lanes) for b in (0, 128)]
        total_0 = inc[BLOCK - 1 : BLOCK]
        total_1 = inc[TOKENS - 1 : TOKENS]
        here = slice(i * LANE_TOTAL, i * LANE_TOTAL + LANE_TOTAL)
        own_ref[here, :] = own[0]
        pull_ref[0, here, :] = pull[0]
        pull_ref[1, here, :] = pull[1]
        total_ref[0, 0:1, lanes] = total_0
        total_ref[0, 1:2, lanes] = total_1
        row = pl.multiple_of((base + i) * LANE_TOTAL, LANE_TOTAL)
        send_ref[pl.ds(row, LANE_TOTAL), :] = jnp.exp(total_1) * own[0] + own[1]
        send_ref[pl.ds(HALF_ROWS + row, LANE_TOTAL), :] = jnp.exp(total_0) * pull[1] + pull[0]
        send_ref[pl.ds(2 * HALF_ROWS + base + i, 1), :] = jnp.exp(total_0 + total_1)


def lower_twice():
    rows, cols = iotas()
    return twice((rows >= cols) & (rows // BLOCK == cols // BLOCK))


def theirs_kernel(core_ref, x_ref, down_ref, r_ref, k_ref, v_ref, g_ref, up_ref, speed_ref, smooth_ref, *outs):
    @pl.when(pl.program_id(0) == 0)
    def _():
        smooth_ref[...] = jnp.tanh(mm(x_ref[...], down_ref[...], NN))

    early_steps(1 - core_ref[0], smooth_ref[...].astype(BF16), r_ref, k_ref, v_ref, g_ref, up_ref, speed_ref, *outs)


def mine_kernel(core_ref, smooth_ref, r_ref, k_ref, v_ref, g_ref, up_ref, speed_ref, *rest):
    early_steps(core_ref[0], smooth_ref[...].astype(BF16), r_ref, k_ref, v_ref, g_ref, up_ref, speed_ref, *rest[6:])


def join_kernel(place_ref, mine_ref, other_ref, send_ref):
    first = place_ref[0] == 0

    def both(rows):
        mine = mine_ref[rows, :]
        other = other_ref[rows, :]
        return jnp.where(first, mine, other), jnp.where(first, other, mine)

    for i in range(HALF):
        decay_a, decay_b = both(slice(2 * HALF_ROWS + i, 2 * HALF_ROWS + i + 1))
        decay = decay_a * decay_b
        for q in range(8):
            at = i * LANE_TOTAL + q * 8
            own_a, own_b = both(slice(at, at + 8))
            pull_a, pull_b = both(slice(HALF_ROWS + at, HALF_ROWS + at + 8))
            for way, state in enumerate((decay_b * own_a + own_b, pull_a + decay_a * pull_b)):
                group = way * 80 + i * 8 + q
                slot, place = divmod(group, 5)
                send_ref[slot, place * 8 : place * 8 + 8, :] = state
                send_ref[slot, 40 + place : 41 + place, :] = decay


def scan_kernel(place_ref, in_ref, out_ref):
    count = in_ref.shape[0]
    flip = place_ref[0]

    def step(e, run):
        at = jnp.where(flip > 0, count - 1 - e, e)
        result = []
        for q in range(5):
            out_ref[at, q * 8 : q * 8 + 8, :] = run[q]
            decay = in_ref[at, 40 + q : 41 + q, :]
            result.append(decay * run[q] + in_ref[at, q * 8 : q * 8 + 8, :])
        return tuple(result)

    lax.fori_loop(0, count, step, tuple(jnp.zeros((8, 128), F32) for _ in range(5)))


def part_kernel(place_ref, chip_ref, mine_ref, other_ref, keep_ref, give_ref):
    first = place_ref[0] == 0

    def both(rows):
        mine = mine_ref[rows, :]
        other = other_ref[rows, :]
        return jnp.where(first, mine, other), jnp.where(first, other, mine)

    for i in range(HALF):
        decay_a, decay_b = both(slice(2 * HALF_ROWS + i, 2 * HALF_ROWS + i + 1))
        ahead = slice(i * LANE_TOTAL, i * LANE_TOTAL + LANE_TOTAL)
        behind = slice(HALF_ROWS + i * LANE_TOTAL, HALF_ROWS + i * LANE_TOTAL + LANE_TOTAL)
        start_a = chip_ref[ahead, :]
        end_b = chip_ref[behind, :]
        start_b = decay_a * start_a + jnp.where(first, mine_ref[ahead, :], other_ref[ahead, :])
        end_a = decay_b * end_b + jnp.where(first, other_ref[behind, :], mine_ref[behind, :])
        keep_ref[ahead, :] = jnp.where(first, start_a, start_b)
        give_ref[ahead, :] = jnp.where(first, start_b, start_a)
        keep_ref[behind, :] = jnp.where(first, end_a, end_b)
        give_ref[behind, :] = jnp.where(first, end_b, end_a)


def two(x, low):
    x = x.astype(F32)
    zero = jnp.zeros_like(x)
    return jnp.concatenate([jnp.where(low, x, zero), jnp.where(low, zero, x)], axis=0).astype(BF16)


def corners(state, low_lanes):
    zero = jnp.zeros_like(state)
    return jnp.concatenate([jnp.where(low_lanes, state, zero), jnp.where(low_lanes, zero, state)], axis=0).astype(BF16)


def beside(x):
    return jnp.concatenate([x[:TOKENS], x[TOKENS:]], axis=1)


def blocks(left, right_0, right_1, dims):
    return mm(apart(left), jnp.concatenate([right_0, right_1], axis=1 if dims == NT else 0), dims)


def near_kernel(core_ref, r_ref, k_ref, v_ref, g_ref, bonus_ref, log_ref,
                fade_ref, mixed_ref, gr_ref, gk_ref, gv_ref, row_ref):
    rows, cols = iotas()
    same = rows // BLOCK == cols // BLOCK
    strict = (rows > cols) & same
    strict_2 = jnp.concatenate([strict, strict], axis=0)
    before = twice(strict)
    heads = ((rows // LANE_TOTAL) == (cols // LANE_TOTAL)).astype(F32).astype(BF16)
    heads_2 = jnp.concatenate([heads, heads], axis=0)
    low = cols < LANE_TOTAL

    def head_sums(x):
        hi = x.astype(BF16)
        rest = (x - hi.astype(F32)).astype(BF16)
        return mm(jnp.concatenate([hi, rest], axis=1), heads_2, NN)

    step = pl.program_id(0)
    parts = []
    incs = sum_rows(lower_twice(), log_ref[...])
    for i in range(CHUNK):
        p = step * CHUNK + i
        lanes = slice(i * 128, i * 128 + 128)
        v = v_ref[:, lanes]
        g = g_ref[:, lanes]
        rf = r_ref[:, lanes].astype(F32)
        kf = k_ref[:, lanes].astype(F32)
        vf = v.astype(F32)
        gf = g.astype(F32)
        bonus = bonus_ref[pl.ds(p, 1), :]
        inc = incs[:, lanes]
        exc = inc - log_ref[:, lanes]
        middle = per_block(inc, BLOCK // 2 - 1)
        upward = jnp.exp(exc - middle)
        downward = jnp.exp(middle - inc)
        early = (rf * upward).astype(BF16)
        late = (kf * downward).astype(BF16)
        early_2 = two(early, low)
        late_2 = two(late, low)
        v_2 = two(v, low)
        g_2 = two(g, low)
        scores = jnp.where(strict_2, mm(early_2, late, NT), 0.0).astype(BF16)
        products = jnp.where(strict_2, mm(g_2, v, NT), 0.0).astype(BF16)
        present = head_sums(rf * bonus * kf)
        agree = head_sums(vf * gf)
        mixed_ref[:, lanes] = mm(beside(scores), v_2, NN) + present * vf
        gv_ref[:, lanes] = mm(scores, g_2, TN) + present * gf
        r_near = mm(beside(products), late_2, NN)
        k_near = mm(products, early_2, TN)
        gr_ref[:, lanes] = upward * r_near + bonus * kf * agree
        gk_ref[:, lanes] = downward * k_near + bonus * rf * agree
        row_ref[pl.ds(p, 1), :] = jnp.sum(rf * kf * agree, axis=0, keepdims=True)
        r_part = early.astype(F32) * r_near
        k_part = late.astype(F32) * k_near
        parts.append((r_part, k_part))
    r_parts, k_parts = (jnp.concatenate(z, axis=1) for z in zip(*parts))
    fade_ref[...] = sum_rows(before, k_parts - r_parts) - r_parts


def start_and_end(i, start_0, end_1, own_ref, pull_ref, decay_0, decay_1):
    here = slice(i * LANE_TOTAL, i * LANE_TOTAL + LANE_TOTAL)
    start_1 = decay_0 * start_0 + own_ref[here, :]
    end_0 = decay_1 * end_1 + pull_ref[1, here, :]
    return start_0, start_1, end_0, end_1


def slope_steps(v_ref, g_ref, log_ref, total_ref, reached_ref, faded_ref, own_ref, pull_ref, state_ref, fade_ref):
    step = pl.program_id(0)
    rows, cols = iotas()
    before = twice((rows > cols) & (rows // BLOCK == cols // BLOCK))
    low_lanes = cols[:LANE_TOTAL] < LANE_TOTAL

    def rounded(z):
        return z.astype(BF16).astype(F32)

    spread = range(CHUNK)
    lanes = [slice(i * 128, i * 128 + 128) for i in spread]
    here = [slice(i * LANE_TOTAL, i * LANE_TOTAL + LANE_TOTAL) for i in spread]
    decays = jnp.exp(total_ref[0, 0:2, :])
    decay = [(decays[0:1, z], decays[1:2, z]) for z in lanes]
    states = []
    for i in spread:
        row = pl.multiple_of((step * CHUNK + i) * LANE_TOTAL, LANE_TOTAL)
        pair = state_ref[pl.ds(row, LANE_TOTAL), :], state_ref[pl.ds(HALF_ROWS + row, LANE_TOTAL), :]
        states.append(start_and_end(i, *pair, own_ref, pull_ref, *decay[i]))
    sides = [[corners(z, low_lanes) for z in four] for four in states]
    r_starts = jnp.concatenate([blocks(g_ref[:, lanes[i]], sides[i][0], sides[i][1], NN) for i in spread], axis=1)
    k_ends = jnp.concatenate([blocks(v_ref[:, lanes[i]], sides[i][2], sides[i][3], NN) for i in spread], axis=1)
    couples = []
    for i in spread:
        start_0, start_1, end_0, end_1 = (rounded(z) for z in states[i])
        couple_0 = jnp.sum((decay[i][0] * end_0 + pull_ref[0, here[i], :]) * start_0, axis=0, keepdims=True)
        couple_1 = jnp.sum((decay[i][1] * end_1 + pull_ref[1, here[i], :]) * start_1, axis=0, keepdims=True)
        couples.append(jnp.concatenate([jnp.broadcast_to(couple_0, (BLOCK, 128)), jnp.broadcast_to(couple_1, (BLOCK, 128))], axis=0))
    r_part = reached_ref[...].astype(F32) * r_starts
    k_part = faded_ref[...].astype(F32) * k_ends
    fading = jnp.concatenate(couples, axis=1) + sum_rows(before, k_part - r_part) - r_part + fade_ref[...]
    slope = fading * log_ref[...]
    return slope.astype(BF16), jnp.sum(slope, axis=0, keepdims=True)


def slope_kernel(core_ref, v_ref, g_ref, log_ref, total_ref, reached_ref, faded_ref, own_ref, pull_ref, state_ref, fade_ref,
                 slope_ref, sums_ref):
    slope_half, sums = slope_steps(v_ref, g_ref, log_ref, total_ref, reached_ref, faded_ref, own_ref, pull_ref, state_ref, fade_ref)
    slope_ref[...] = slope_half
    for i in range(CHUNK):
        sums_ref[pl.ds(pl.program_id(0) * CHUNK + i, 1), :] = sums[:, i * 128 : i * 128 + 128]


def grads_kernel(core_ref, v_ref, g_ref, log_ref, total_ref, reached_ref, faded_ref, own_ref, pull_ref, state_ref, fade_ref,
                 x_ref, up_ref, smooth_ref, slope_ref, sums_ref, row_ref,
                 keep_ref, give_ref, project_ref, stage_ref, rest_ref, gate_ref, sems):
    core = core_ref[0]
    step = pl.program_id(0)
    smooth = smooth_ref[...]
    gate = smooth.astype(BF16)
    width = CHUNK * 128

    def rows_of(half, at):
        return pl.ds(pl.multiple_of(half * (SPAN // 2) + at * width, 128), width)

    @pl.when(step == 0)
    def _():
        slopes = slope_ref[...]
        stage_ref[1 - core, core] = mm(slopes, gate, TN)
        gate_ref[...] = mm(slopes, up_ref[pl.ds(pl.multiple_of(core * (SPAN // 2), 128), SPAN // 2), :], NN)
        for i in range(HALF):
            rest_ref[core, core, i, 0:1, :] = sums_ref[i : i + 1, :]
            for half in range(2):
                rest_ref[1 - core, half, i, 0:1, :] = row_ref[half * HALF + i : half * HALF + i + 1, :]

    slope_half, sums = slope_steps(v_ref, g_ref, log_ref, total_ref, reached_ref, faded_ref, own_ref, pull_ref, state_ref, fade_ref)
    stage_ref[1 - core, 1 - core, pl.ds(pl.multiple_of(step * width, 128), width), :] = mm(slope_half, gate, TN)
    for i in range(CHUNK):
        rest_ref[core, 1 - core, step * CHUNK + i, 0:1, :] = sums[:, i * 128 : i * 128 + 128]
    gate_ref[...] += mm(slope_half, up_ref[rows_of(1 - core, step), :], NN)

    @pl.when(step == HALF_STEPS - 1)
    def _():
        project_grad = (gate_ref[...] * (1.0 - smooth * smooth)).astype(BF16)
        project_ref[...] = project_grad
        for c in range(2):
            stage_ref[core, c] = mm(x_ref[:, c * SPAN // 2 : (c + 1) * SPAN // 2], project_grad, TN)
        copies = []
        for j, ref in enumerate((keep_ref, give_ref)):
            for half in range(2):
                tiles = stage_ref.at[j, half].reshape(32, 40, 128)
                copies.append(pltpu.make_async_copy(tiles, ref.at[:, half, pl.ds(0, 40), :], sems.at[j, half, 0]))
                copies.append(pltpu.make_async_copy(rest_ref.at[j, half], ref.at[pl.ds(0, HALF), half, pl.ds(40, 8), :], sems.at[j, half, 1]))
        for copy in copies:
            copy.start()
        for copy in copies:
            copy.wait()


def last_kernel(core_ref, v_ref, g_ref, down_ref, log_ref, reached_ref, faded_ref, own_ref, pull_ref, mine_ref, other_ref,
                near_mixed_ref, near_gr_ref, near_gk_ref, near_gv_ref, project_ref,
                mixed_ref, gr_ref, gk_ref, gv_ref, gx_ref):
    _, cols = iotas()
    low_lanes = cols[:LANE_TOTAL] < LANE_TOTAL
    project_grad = project_ref[...]
    core = core_ref[0]
    step = pl.program_id(0)
    incs = sum_rows(lower_twice(), log_ref[...])
    for i in range(CHUNK):
        lanes = slice(i * 128, i * 128 + 128)
        inc = incs[:, lanes]
        decay_0 = jnp.exp(inc[BLOCK - 1 : BLOCK])
        decay_1 = jnp.exp(inc[TOKENS - 1 : TOKENS])
        row = pl.multiple_of((step % HALF_STEPS * CHUNK + i) * LANE_TOTAL, LANE_TOTAL)
        pair = [jnp.where(step // HALF_STEPS == core, mine_ref[at, :], other_ref[at, :])
                for at in (pl.ds(row, LANE_TOTAL), pl.ds(HALF_ROWS + row, LANE_TOTAL))]
        states = start_and_end(i, *pair, own_ref, pull_ref, decay_0, decay_1)
        s_0, s_1, e_0, e_1 = (corners(z, low_lanes) for z in states)
        entering = jnp.exp(inc - log_ref[:, lanes])
        leaving = jnp.exp(per_block(inc, BLOCK - 1) - inc)
        mixed_ref[:, lanes] = (near_mixed_ref[:, lanes] + blocks(reached_ref[:, lanes], s_0, s_1, NT)).astype(BF16)
        gv_ref[:, lanes] = (near_gv_ref[:, lanes] + blocks(faded_ref[:, lanes], e_0, e_1, NT)).astype(BF16)
        gr_ref[:, lanes] = (near_gr_ref[:, lanes] + entering * blocks(g_ref[:, lanes], s_0, s_1, NN)).astype(BF16)
        gk_ref[:, lanes] = (near_gk_ref[:, lanes] + leaving * blocks(v_ref[:, lanes], e_0, e_1, NN)).astype(BF16)
        gx_ref[:, lanes] = mm(project_grad, down_ref[lanes, :], NT).astype(BF16)


def final_kernel(core_ref, mine_ref, other_ref, a_ref, b_ref, a_row_ref, b_row_ref, sems):
    first = core_ref[0] == 0

    def send(x_ref, y_ref):
        copies = [pltpu.make_async_copy(z.at[:, pl.ds(0, 40), :], ref, sems.at[j]) for j, (z, ref) in enumerate(((x_ref, a_ref), (y_ref, b_ref)))]
        for copy in copies:
            copy.start()
        for i in range(HALF):
            a_row_ref[i : i + 1, :] = x_ref[i, 40:41, :]
            b_row_ref[i : i + 1, :] = y_ref[i, 40:41, :]
        for copy in copies:
            copy.wait()

    pl.when(first)(lambda: send(mine_ref, other_ref))
    pl.when(jnp.logical_not(first))(lambda: send(other_ref, mine_ref))


def final_call():
    vmem = pl.BlockSpec(memory_space=pltpu.VMEM)
    hbm = pl.BlockSpec(memory_space=pl.ANY)
    return pl.pallas_call(
        final_kernel,
        in_specs=[pl.BlockSpec(memory_space=pltpu.SMEM), vmem, vmem],
        out_specs=[hbm, hbm, vmem, vmem],
        out_shape=[jax.ShapeDtypeStruct(z, F32) for z in ((32, 40, 128), (32, 40, 128), (HALF, 128), (HALF, 128))],
        scratch_shapes=[pltpu.SemaphoreType.DMA((2,))],
        compiler_params=pltpu.CompilerParams(vmem_limit_bytes=8 * 1024 * 1024),
        name="final",
    )


def call(kernel, outs, count=0):
    more = {}
    if count:
        more["in_specs"] = [pl.BlockSpec(memory_space=pltpu.SMEM)] + [pl.BlockSpec(memory_space=pltpu.VMEM)] * (count - 1)
    return pl.pallas_call(
        kernel,
        out_shape=[jax.ShapeDtypeStruct(s, d) for s, d in outs],
        compiler_params=pltpu.CompilerParams(vmem_limit_bytes=8 * 1024 * 1024),
        **more,
    )


WIDE = ((TOKENS, SPAN), lambda at: pl.BlockSpec((TOKENS, CHUNK * 128), lambda s, core: (0, at(s, core))))
WEIGHT = ((SPAN, 128), lambda at: pl.BlockSpec((CHUNK * 128, 128), lambda s, core: (at(s, core), 0)))
STATE = ((PAIRS * LANE_TOTAL, 128), lambda at: pl.BlockSpec((CHUNK * LANE_TOTAL, 128), lambda s, core: (at(s, core), 0)))
STATES = ((2, PAIRS * LANE_TOTAL, 128), lambda at: pl.BlockSpec((2, CHUNK * LANE_TOTAL, 128), lambda s, core: (0, at(s, core), 0)))


def whole(*shape):
    return (shape, lambda at: pl.BlockSpec(shape, lambda s, core: (0,) * len(shape)))


def kept(*shape):
    return (shape, lambda at: pl.BlockSpec(memory_space=pl.ANY))


TOTAL = ((STEPS, 2, CHUNK * 128), lambda at: pl.BlockSpec((1, 2, CHUNK * 128), lambda s, core: (at(s, core), 0, 0)))


def in_steps(kernel, ins, outs, scratch=(), at=lambda s, core: s, steps=STEPS, aliases=None, flops=10 ** 9):
    return pl.pallas_call(
        kernel,
        grid_spec=pltpu.PrefetchScalarGridSpec(
            num_scalar_prefetch=1,
            grid=(steps,),
            in_specs=[spec(at) for _, spec in ins],
            out_specs=[spec(at) for (_, spec), _ in outs],
            scratch_shapes=list(scratch),
        ),
        out_shape=[jax.ShapeDtypeStruct(shape, dtype) if shape in FREE else pltpu.HBM(shape, dtype) for (shape, spec), dtype in outs],
        compiler_params=pltpu.CompilerParams(vmem_limit_bytes=VMEM_LIMIT * 1024 * 1024, dimension_semantics=("arbitrary",)),
        cost_estimate=pl.CostEstimate(flops=flops, bytes_accessed=flops // 1000, transcendentals=0),
        input_output_aliases=aliases or {},
    )


ROWS = whole(PAIRS, 128)
SQUARE = whole(TOKENS, 128)
PART = whole(2 * HALF_ROWS + 16, 128)
STATE_PART = whole(2 * HALF_ROWS, 128)
HALF_WIDE = ((TOKENS, SPAN // 2), lambda at: pl.BlockSpec((TOKENS, CHUNK * 128), lambda s, core: (0, s)))
EARLY = [(WIDE, F32), (WIDE, BF16), (WIDE, BF16), (STATE, F32), (STATES, F32), (TOTAL, F32)]
SLOPE = [WIDE, WIDE, WIDE, TOTAL, WIDE, WIDE, STATE, STATES, STATE_PART, WIDE]


def mine_half(s, core):
    return core[0] * HALF_STEPS + s


def their_half(s, core):
    return (1 - core[0]) * HALF_STEPS + s


def theirs_call():
    return in_steps(
        theirs_kernel, [whole(TOKENS, SPAN), whole(SPAN, 128), WIDE, WIDE, WIDE, WIDE, WEIGHT, ROWS],
        [(SQUARE, F32)] + EARLY + [(PART, F32)], at=their_half, steps=HALF_STEPS,
    )


def mine_call():
    return in_steps(
        mine_kernel, [SQUARE, WIDE, WIDE, WIDE, WIDE, WEIGHT, ROWS] + [kept(*z[0][0]) for z in EARLY],
        EARLY + [(PART, F32)], at=mine_half, steps=HALF_STEPS, aliases={8 + j: j for j in range(len(EARLY))},
    )


def near_call():
    return in_steps(near_kernel, [WIDE] * 4 + [ROWS, WIDE], [(WIDE, F32)] * 5 + [(ROWS, F32)])


def slope_call():
    return in_steps(slope_kernel, SLOPE, [(HALF_WIDE, BF16), (whole(HALF, 128), F32)], at=mine_half, steps=HALF_STEPS)


def grads_call():
    return in_steps(
        grads_kernel, SLOPE + [whole(TOKENS, SPAN), whole(SPAN, 128), SQUARE, whole(TOKENS, SPAN // 2), whole(HALF, 128), ROWS],
        [(kept(32, 2, 48, 128), F32), (kept(32, 2, 48, 128), F32), (SQUARE, BF16)],
        (pltpu.VMEM((2, 2, SPAN // 2, 128), F32), pltpu.VMEM((2, 2, HALF, 8, 128), F32), pltpu.VMEM((TOKENS, 128), F32),
         pltpu.SemaphoreType.DMA((2, 2, 2))),
        at=their_half, steps=HALF_STEPS,
    )


def last_call():
    return in_steps(
        last_kernel,
        [WIDE, WIDE, WEIGHT, WIDE, WIDE, WIDE, STATE, STATES, STATE_PART, STATE_PART, WIDE, WIDE, WIDE, WIDE, SQUARE],
        [(WIDE, BF16)] * 5,
    )


def exchange(x, axes):
    return lax.all_to_all(x, axes, 0, 0, tiled=True)


def swap(x):
    return lax.ppermute(x, CORE, [(0, 1), (1, 0)])


def far(*arrays):
    return [pltpu.with_memory_space_constraint(z, pltpu.HBM) for z in arrays]


def inside(r, k, v, x, g, down, up, speed, bonus):
    r, k, v, x, g = (z[0] for z in (r, k, v, x, g))
    speed = speed.reshape(PAIRS, 128)
    bonus = bonus.reshape(PAIRS, 128)
    r, k, v, x, g, down, up, speed, bonus = far(r, k, v, x, g, down, up, speed, bonus)
    core = lax.axis_index(CORE).astype(jnp.int32)[None]
    flip = (lax.axis_index(CHIPS) // 16).astype(jnp.int32)[None]
    smooth, *early, theirs = theirs_call()(core, x, down, r, k, v, g, up, speed)
    (smooth,) = far(smooth)
    other = swap(theirs)
    *early, mine = mine_call()(core, smooth, r, k, v, g, up, speed, *far(*early))
    log_decay, reached, faded, own, pull, total = far(*early)
    (joined,) = call(join_kernel, [((32, 48, 128), F32)], 3)(core, mine, other)
    there = exchange(joined, CHIPS)
    near = near_call()(core, r, k, v, g, bonus, log_decay)
    fade, near_mixed, near_gr, near_gk, near_gv, bonus_rows = far(*near)
    (scanned,) = call(scan_kernel, [((32, 40, 128), F32)], 2)(flip, there)
    chip = exchange(scanned, CHIPS).reshape(2 * HALF_ROWS, 128)
    keep, give = call(part_kernel, [((2 * HALF_ROWS, 128), F32)] * 2, 4)(core, chip, mine, other)
    got = swap(give)
    slope_mine, sums_mine = far(*slope_call()(core, v, g, log_decay, total, reached, faded, own, pull, keep, fade))
    held, given, project_grad = grads_call()(core, v, g, log_decay, total, reached, faded, own, pull, got, fade,
                                             x, up, smooth, slope_mine, sums_mine, bonus_rows)
    (project_grad,) = far(project_grad)
    grads = (held + swap(given)).reshape(64, 48, 128)
    pieces = exchange(grads, CHIPS + ("dp",))
    mixed, gr, gk, gv, gx = last_call()(core, v, g, down, log_decay, reached, faded, own, pull, keep, got,
                                        near_mixed, near_gr, near_gk, near_gv, project_grad)
    summed = jnp.sum(pieces, axis=0)
    matrix = exchange(jnp.broadcast_to(summed[None], (32, 48, 128)), CHIPS)
    a, b, a_row, b_row = final_call()(core, matrix, swap(matrix))
    return (mixed[None], gr[None], gk[None], gv[None], gx[None],
            a.reshape(SPAN // 2, 128), b.reshape(SPAN // 2, 128), a_row.reshape(SPAN // 2), b_row.reshape(SPAN // 2))


def solution(mesh):
    split = Mesh(mesh.devices.reshape(4, 2, 4, 2, mesh.shape["dp"]), SEQ + ("dp",))
    tokens = P("dp", SEQ, None)
    return jax.shard_map(
        inside,
        mesh=split,
        in_specs=(tokens,) * 5 + (P(),) * 4,
        out_specs=(tokens,) * 5 + (P("dp", None), P("dp", None), P("dp"), P("dp")),
        check_vma=False,
    )
```

```python
import jax
import jax.numpy as jnp
from jax import lax
from jax.experimental import pallas as pl
from jax.experimental.pallas import tpu as pltpu
from jax.sharding import Mesh
from jax.sharding import PartitionSpec as P


LANE_TOTAL = 64
BLOCK = 64
TOKENS = 128
PAIRS = 20
SPAN = 2560
SEQ = ("seq_0", "seq_1", "seq_2", "seq_3")
CHIPS = SEQ[:3]
CORE = SEQ[3]
HALF = 10
HALF_ROWS = 640
CHUNK = 10
HALF_STEPS = HALF // CHUNK
STEPS = 2 * HALF_STEPS
VMEM_LIMIT = 24
FREE = ((32, 2, 48, 128), (1296, 128))
F32 = jnp.float32
BF16 = jnp.bfloat16
NN = (((1,), (0,)), ((), ()))
NT = (((1,), (1,)), ((), ()))
TN = (((0,), (0,)), ((), ()))


def mm(left, right, dims):
    return lax.dot_general(left, right, dims, preferred_element_type=F32)


def iotas():
    rows = lax.broadcasted_iota(jnp.int32, (TOKENS, 128), 0)
    cols = lax.broadcasted_iota(jnp.int32, (TOKENS, 128), 1)
    return rows, cols


def sum_rows(matrix_2, x):
    hi = x.astype(BF16)
    low = (x - hi.astype(F32)).astype(BF16)
    return mm(matrix_2, jnp.concatenate([hi, low], axis=0), NN)


def twice(mask):
    one = mask.astype(F32).astype(BF16)
    return jnp.concatenate([one, one], axis=1)


def apart(x):
    zero = jnp.zeros((BLOCK, x.shape[1]), x.dtype)
    top = jnp.concatenate([x[:BLOCK], zero], axis=1)
    bottom = jnp.concatenate([zero, x[BLOCK:]], axis=1)
    return jnp.concatenate([top, bottom], axis=0)


def per_block(row_of, first):
    top = jnp.broadcast_to(row_of[first : first + 1], (BLOCK, 128))
    bottom = jnp.broadcast_to(row_of[BLOCK + first : BLOCK + first + 1], (BLOCK, 128))
    return jnp.concatenate([top, bottom], axis=0)


def pack(full, low_lanes):
    return jnp.where(low_lanes, full[:LANE_TOTAL], full[LANE_TOTAL:])


def early_steps(half, gate, r_ref, k_ref, v_ref, g_ref, up_ref, speed_ref,
                log_ref, reached_ref, faded_ref, own_ref, pull_ref, total_ref, send_ref):
    step = pl.program_id(0)
    lower = lower_twice()
    low_lanes = iotas()[1][:LANE_TOTAL] < LANE_TOTAL
    base = step * CHUNK
    speed = jnp.concatenate([speed_ref[pl.ds(half * HALF + base + i, 1), :] for i in range(CHUNK)], axis=1)
    log_decays = -speed * jnp.exp(mm(gate, up_ref[...], NT))
    incs = sum_rows(lower, log_decays)
    log_ref[...] = log_decays
    for i in range(CHUNK):
        lanes = slice(i * 128, i * 128 + 128)
        inc = incs[:, lanes]
        exc = inc - log_decays[:, lanes]
        total = per_block(inc, BLOCK - 1)
        reached = (r_ref[:, lanes].astype(F32) * jnp.exp(exc)).astype(BF16)
        faded = (k_ref[:, lanes].astype(F32) * jnp.exp(total - inc)).astype(BF16)
        reached_ref[:, lanes] = reached
        faded_ref[:, lanes] = faded
        owns = mm(v_ref[:, lanes], apart(faded), TN)
        pulls = mm(g_ref[:, lanes], apart(reached), TN)
        own = [pack(owns[:, b : b + 128], low_lanes) for b in (0, 128)]
        pull = [pack(pulls[:, b : b + 128], low_lanes) for b in (0, 128)]
        total_0 = inc[BLOCK - 1 : BLOCK]
        total_1 = inc[TOKENS - 1 : TOKENS]
        here = slice(i * LANE_TOTAL, i * LANE_TOTAL + LANE_TOTAL)
        own_ref[here, :] = own[0]
        pull_ref[0, here, :] = pull[0]
        pull_ref[1, here, :] = pull[1]
        total_ref[0, 0:1, lanes] = total_0
        total_ref[0, 1:2, lanes] = total_1
        row = pl.multiple_of((base + i) * LANE_TOTAL, LANE_TOTAL)
        send_ref[pl.ds(row, LANE_TOTAL), :] = jnp.exp(total_1) * own[0] + own[1]
        send_ref[pl.ds(HALF_ROWS + row, LANE_TOTAL), :] = jnp.exp(total_0) * pull[1] + pull[0]
        send_ref[pl.ds(2 * HALF_ROWS + base + i, 1), :] = jnp.exp(total_0 + total_1)


def lower_twice():
    rows, cols = iotas()
    return twice((rows >= cols) & (rows // BLOCK == cols // BLOCK))


def theirs_kernel(core_ref, x_ref, down_ref, r_ref, k_ref, v_ref, g_ref, up_ref, speed_ref, smooth_ref, *outs):
    @pl.when(pl.program_id(0) == 0)
    def _():
        smooth_ref[...] = jnp.tanh(mm(x_ref[...], down_ref[...], NN))

    early_steps(1 - core_ref[0], smooth_ref[...].astype(BF16), r_ref, k_ref, v_ref, g_ref, up_ref, speed_ref, *outs)


def mine_kernel(core_ref, smooth_ref, r_ref, k_ref, v_ref, g_ref, up_ref, speed_ref, *rest):
    early_steps(core_ref[0], smooth_ref[...].astype(BF16), r_ref, k_ref, v_ref, g_ref, up_ref, speed_ref, *rest[6:])


def join_kernel(place_ref, mine_ref, other_ref, send_ref):
    first = place_ref[0] == 0

    def both(rows):
        mine = mine_ref[rows, :]
        other = other_ref[rows, :]
        return jnp.where(first, mine, other), jnp.where(first, other, mine)

    for i in range(HALF):
        decay_a, decay_b = both(slice(2 * HALF_ROWS + i, 2 * HALF_ROWS + i + 1))
        decay = decay_a * decay_b
        for q in range(8):
            at = i * LANE_TOTAL + q * 8
            own_a, own_b = both(slice(at, at + 8))
            pull_a, pull_b = both(slice(HALF_ROWS + at, HALF_ROWS + at + 8))
            for way, state in enumerate((decay_b * own_a + own_b, pull_a + decay_a * pull_b)):
                group = way * 80 + i * 8 + q
                slot, place = divmod(group, 5)
                send_ref[slot, place * 8 : place * 8 + 8, :] = state
                send_ref[slot, 40 + place : 41 + place, :] = decay


def scan_kernel(place_ref, in_ref, out_ref):
    count = in_ref.shape[0]
    flip = place_ref[0]

    def step(e, run):
        at = jnp.where(flip > 0, count - 1 - e, e)
        result = []
        for q in range(5):
            out_ref[at, q * 8 : q * 8 + 8, :] = run[q]
            decay = in_ref[at, 40 + q : 41 + q, :]
            result.append(decay * run[q] + in_ref[at, q * 8 : q * 8 + 8, :])
        return tuple(result)

    lax.fori_loop(0, count, step, tuple(jnp.zeros((8, 128), F32) for _ in range(5)))


def part_kernel(place_ref, chip_ref, mine_ref, other_ref, keep_ref, give_ref):
    first = place_ref[0] == 0

    def both(rows):
        mine = mine_ref[rows, :]
        other = other_ref[rows, :]
        return jnp.where(first, mine, other), jnp.where(first, other, mine)

    for i in range(HALF):
        decay_a, decay_b = both(slice(2 * HALF_ROWS + i, 2 * HALF_ROWS + i + 1))
        ahead = slice(i * LANE_TOTAL, i * LANE_TOTAL + LANE_TOTAL)
        behind = slice(HALF_ROWS + i * LANE_TOTAL, HALF_ROWS + i * LANE_TOTAL + LANE_TOTAL)
        start_a = chip_ref[ahead, :]
        end_b = chip_ref[behind, :]
        start_b = decay_a * start_a + jnp.where(first, mine_ref[ahead, :], other_ref[ahead, :])
        end_a = decay_b * end_b + jnp.where(first, other_ref[behind, :], mine_ref[behind, :])
        keep_ref[ahead, :] = jnp.where(first, start_a, start_b)
        give_ref[ahead, :] = jnp.where(first, start_b, start_a)
        keep_ref[behind, :] = jnp.where(first, end_a, end_b)
        give_ref[behind, :] = jnp.where(first, end_b, end_a)


def two(x, low):
    x = x.astype(F32)
    zero = jnp.zeros_like(x)
    return jnp.concatenate([jnp.where(low, x, zero), jnp.where(low, zero, x)], axis=0).astype(BF16)


def corners(state, low_lanes):
    zero = jnp.zeros_like(state)
    return jnp.concatenate([jnp.where(low_lanes, state, zero), jnp.where(low_lanes, zero, state)], axis=0).astype(BF16)


def beside(x):
    return jnp.concatenate([x[:TOKENS], x[TOKENS:]], axis=1)


def blocks(left, right_0, right_1, dims):
    return mm(apart(left), jnp.concatenate([right_0, right_1], axis=1 if dims == NT else 0), dims)


def near_kernel(core_ref, r_ref, k_ref, v_ref, g_ref, bonus_ref, log_ref,
                fade_ref, mixed_ref, gr_ref, gk_ref, gv_ref, row_ref):
    rows, cols = iotas()
    same = rows // BLOCK == cols // BLOCK
    strict = (rows > cols) & same
    strict_2 = jnp.concatenate([strict, strict], axis=0)
    before = twice(strict)
    heads = ((rows // LANE_TOTAL) == (cols // LANE_TOTAL)).astype(F32).astype(BF16)
    heads_2 = jnp.concatenate([heads, heads], axis=0)
    low = cols < LANE_TOTAL

    def head_sums(x):
        hi = x.astype(BF16)
        rest = (x - hi.astype(F32)).astype(BF16)
        return mm(jnp.concatenate([hi, rest], axis=1), heads_2, NN)

    step = pl.program_id(0)
    parts = []
    incs = sum_rows(lower_twice(), log_ref[...])
    for i in range(CHUNK):
        p = step * CHUNK + i
        lanes = slice(i * 128, i * 128 + 128)
        v = v_ref[:, lanes]
        g = g_ref[:, lanes]
        rf = r_ref[:, lanes].astype(F32)
        kf = k_ref[:, lanes].astype(F32)
        vf = v.astype(F32)
        gf = g.astype(F32)
        bonus = bonus_ref[pl.ds(p, 1), :]
        inc = incs[:, lanes]
        exc = inc - log_ref[:, lanes]
        middle = per_block(inc, BLOCK // 2 - 1)
        upward = jnp.exp(exc - middle)
        downward = jnp.exp(middle - inc)
        early = (rf * upward).astype(BF16)
        late = (kf * downward).astype(BF16)
        early_2 = two(early, low)
        late_2 = two(late, low)
        v_2 = two(v, low)
        g_2 = two(g, low)
        scores = jnp.where(strict_2, mm(early_2, late, NT), 0.0).astype(BF16)
        products = jnp.where(strict_2, mm(g_2, v, NT), 0.0).astype(BF16)
        present = head_sums(rf * bonus * kf)
        agree = head_sums(vf * gf)
        mixed_ref[:, lanes] = mm(beside(scores), v_2, NN) + present * vf
        gv_ref[:, lanes] = mm(scores, g_2, TN) + present * gf
        r_near = mm(beside(products), late_2, NN)
        k_near = mm(products, early_2, TN)
        gr_ref[:, lanes] = upward * r_near + bonus * kf * agree
        gk_ref[:, lanes] = downward * k_near + bonus * rf * agree
        row_ref[pl.ds(p, 1), :] = jnp.sum(rf * kf * agree, axis=0, keepdims=True)
        r_part = early.astype(F32) * r_near
        k_part = late.astype(F32) * k_near
        parts.append((r_part, k_part))
    r_parts, k_parts = (jnp.concatenate(z, axis=1) for z in zip(*parts))
    fade_ref[...] = sum_rows(before, k_parts - r_parts) - r_parts


def start_and_end(i, start_0, end_1, own_ref, pull_ref, decay_0, decay_1):
    here = slice(i * LANE_TOTAL, i * LANE_TOTAL + LANE_TOTAL)
    start_1 = decay_0 * start_0 + own_ref[here, :]
    end_0 = decay_1 * end_1 + pull_ref[1, here, :]
    return start_0, start_1, end_0, end_1


def slope_steps(v_ref, g_ref, log_ref, total_ref, reached_ref, faded_ref, own_ref, pull_ref, state_ref, fade_ref):
    step = pl.program_id(0)
    rows, cols = iotas()
    before = twice((rows > cols) & (rows // BLOCK == cols // BLOCK))
    low_lanes = cols[:LANE_TOTAL] < LANE_TOTAL

    def rounded(z):
        return z.astype(BF16).astype(F32)

    spread = range(CHUNK)
    lanes = [slice(i * 128, i * 128 + 128) for i in spread]
    here = [slice(i * LANE_TOTAL, i * LANE_TOTAL + LANE_TOTAL) for i in spread]
    decays = jnp.exp(total_ref[0, 0:2, :])
    decay = [(decays[0:1, z], decays[1:2, z]) for z in lanes]
    states = []
    for i in spread:
        row = pl.multiple_of((step * CHUNK + i) * LANE_TOTAL, LANE_TOTAL)
        pair = state_ref[pl.ds(row, LANE_TOTAL), :], state_ref[pl.ds(HALF_ROWS + row, LANE_TOTAL), :]
        states.append(start_and_end(i, *pair, own_ref, pull_ref, *decay[i]))
    sides = [[corners(z, low_lanes) for z in four] for four in states]
    r_starts = jnp.concatenate([blocks(g_ref[:, lanes[i]], sides[i][0], sides[i][1], NN) for i in spread], axis=1)
    k_ends = jnp.concatenate([blocks(v_ref[:, lanes[i]], sides[i][2], sides[i][3], NN) for i in spread], axis=1)
    couples = []
    for i in spread:
        start_0, start_1, end_0, end_1 = (rounded(z) for z in states[i])
        couple_0 = jnp.sum((decay[i][0] * end_0 + pull_ref[0, here[i], :]) * start_0, axis=0, keepdims=True)
        couple_1 = jnp.sum((decay[i][1] * end_1 + pull_ref[1, here[i], :]) * start_1, axis=0, keepdims=True)
        couples.append(jnp.concatenate([jnp.broadcast_to(couple_0, (BLOCK, 128)), jnp.broadcast_to(couple_1, (BLOCK, 128))], axis=0))
    r_part = reached_ref[...].astype(F32) * r_starts
    k_part = faded_ref[...].astype(F32) * k_ends
    fading = jnp.concatenate(couples, axis=1) + sum_rows(before, k_part - r_part) - r_part + fade_ref[...]
    slope = fading * log_ref[...]
    return slope.astype(BF16), jnp.sum(slope, axis=0, keepdims=True)


def slope_kernel(core_ref, v_ref, g_ref, log_ref, total_ref, reached_ref, faded_ref, own_ref, pull_ref, state_ref, fade_ref,
                 slope_ref, sums_ref):
    slope_half, sums = slope_steps(v_ref, g_ref, log_ref, total_ref, reached_ref, faded_ref, own_ref, pull_ref, state_ref, fade_ref)
    slope_ref[...] = slope_half
    for i in range(CHUNK):
        sums_ref[pl.ds(pl.program_id(0) * CHUNK + i, 1), :] = sums[:, i * 128 : i * 128 + 128]


def grads_kernel(core_ref, v_ref, g_ref, log_ref, total_ref, reached_ref, faded_ref, own_ref, pull_ref, state_ref, fade_ref,
                 x_ref, up_ref, smooth_ref, slope_ref, sums_ref, row_ref,
                 keep_ref, give_ref, project_ref, stage_ref, rest_ref, gate_ref, sems):
    core = core_ref[0]
    step = pl.program_id(0)
    smooth = smooth_ref[...]
    gate = smooth.astype(BF16)
    width = CHUNK * 128

    def rows_of(half, at):
        return pl.ds(pl.multiple_of(half * (SPAN // 2) + at * width, 128), width)

    @pl.when(step == 0)
    def _():
        slopes = slope_ref[...]
        stage_ref[1 - core, core] = mm(slopes, gate, TN)
        gate_ref[...] = mm(slopes, up_ref[pl.ds(pl.multiple_of(core * (SPAN // 2), 128), SPAN // 2), :], NN)
        for i in range(HALF):
            rest_ref[core, core, i, 0:1, :] = sums_ref[i : i + 1, :]
            for half in range(2):
                rest_ref[1 - core, half, i, 0:1, :] = row_ref[half * HALF + i : half * HALF + i + 1, :]

    slope_half, sums = slope_steps(v_ref, g_ref, log_ref, total_ref, reached_ref, faded_ref, own_ref, pull_ref, state_ref, fade_ref)
    stage_ref[1 - core, 1 - core, pl.ds(pl.multiple_of(step * width, 128), width), :] = mm(slope_half, gate, TN)
    for i in range(CHUNK):
        rest_ref[core, 1 - core, step * CHUNK + i, 0:1, :] = sums[:, i * 128 : i * 128 + 128]
    gate_ref[...] += mm(slope_half, up_ref[rows_of(1 - core, step), :], NN)

    @pl.when(step == HALF_STEPS - 1)
    def _():
        project_grad = (gate_ref[...] * (1.0 - smooth * smooth)).astype(BF16)
        project_ref[...] = project_grad
        for c in range(2):
            stage_ref[core, c] = mm(x_ref[:, c * SPAN // 2 : (c + 1) * SPAN // 2], project_grad, TN)
        copies = []
        for j, ref in enumerate((keep_ref, give_ref)):
            for half in range(2):
                tiles = stage_ref.at[j, half].reshape(32, 40, 128)
                copies.append(pltpu.make_async_copy(tiles, ref.at[:, half, pl.ds(0, 40), :], sems.at[j, half, 0]))
                copies.append(pltpu.make_async_copy(rest_ref.at[j, half], ref.at[pl.ds(0, HALF), half, pl.ds(40, 8), :], sems.at[j, half, 1]))
        for copy in copies:
            copy.start()
        for copy in copies:
            copy.wait()


def last_kernel(core_ref, v_ref, g_ref, down_ref, log_ref, reached_ref, faded_ref, own_ref, pull_ref, mine_ref, other_ref,
                near_mixed_ref, near_gr_ref, near_gk_ref, near_gv_ref, project_ref,
                mixed_ref, gr_ref, gk_ref, gv_ref, gx_ref):
    _, cols = iotas()
    low_lanes = cols[:LANE_TOTAL] < LANE_TOTAL
    project_grad = project_ref[...]
    core = core_ref[0]
    step = pl.program_id(0)
    incs = sum_rows(lower_twice(), log_ref[...])
    for i in range(CHUNK):
        lanes = slice(i * 128, i * 128 + 128)
        inc = incs[:, lanes]
        decay_0 = jnp.exp(inc[BLOCK - 1 : BLOCK])
        decay_1 = jnp.exp(inc[TOKENS - 1 : TOKENS])
        row = pl.multiple_of((step % HALF_STEPS * CHUNK + i) * LANE_TOTAL, LANE_TOTAL)
        pair = [jnp.where(step // HALF_STEPS == core, mine_ref[at, :], other_ref[at, :])
                for at in (pl.ds(row, LANE_TOTAL), pl.ds(HALF_ROWS + row, LANE_TOTAL))]
        states = start_and_end(i, *pair, own_ref, pull_ref, decay_0, decay_1)
        s_0, s_1, e_0, e_1 = (corners(z, low_lanes) for z in states)
        entering = jnp.exp(inc - log_ref[:, lanes])
        leaving = jnp.exp(per_block(inc, BLOCK - 1) - inc)
        mixed_ref[:, lanes] = (near_mixed_ref[:, lanes] + blocks(reached_ref[:, lanes], s_0, s_1, NT)).astype(BF16)
        gv_ref[:, lanes] = (near_gv_ref[:, lanes] + blocks(faded_ref[:, lanes], e_0, e_1, NT)).astype(BF16)
        gr_ref[:, lanes] = (near_gr_ref[:, lanes] + entering * blocks(g_ref[:, lanes], s_0, s_1, NN)).astype(BF16)
        gk_ref[:, lanes] = (near_gk_ref[:, lanes] + leaving * blocks(v_ref[:, lanes], e_0, e_1, NN)).astype(BF16)
        gx_ref[:, lanes] = mm(project_grad, down_ref[lanes, :], NT).astype(BF16)


def final_kernel(core_ref, mine_ref, other_ref, a_ref, b_ref, a_row_ref, b_row_ref, sems):
    first = core_ref[0] == 0

    def send(x_ref, y_ref):
        copies = [pltpu.make_async_copy(z.at[:, pl.ds(0, 40), :], ref, sems.at[j]) for j, (z, ref) in enumerate(((x_ref, a_ref), (y_ref, b_ref)))]
        for copy in copies:
            copy.start()
        for i in range(HALF):
            a_row_ref[i : i + 1, :] = x_ref[i, 40:41, :]
            b_row_ref[i : i + 1, :] = y_ref[i, 40:41, :]
        for copy in copies:
            copy.wait()

    pl.when(first)(lambda: send(mine_ref, other_ref))
    pl.when(jnp.logical_not(first))(lambda: send(other_ref, mine_ref))


def final_call():
    vmem = pl.BlockSpec(memory_space=pltpu.VMEM)
    hbm = pl.BlockSpec(memory_space=pl.ANY)
    return pl.pallas_call(
        final_kernel,
        in_specs=[pl.BlockSpec(memory_space=pltpu.SMEM), vmem, vmem],
        out_specs=[hbm, hbm, vmem, vmem],
        out_shape=[jax.ShapeDtypeStruct(z, F32) for z in ((32, 40, 128), (32, 40, 128), (HALF, 128), (HALF, 128))],
        scratch_shapes=[pltpu.SemaphoreType.DMA((2,))],
        compiler_params=pltpu.CompilerParams(vmem_limit_bytes=8 * 1024 * 1024),
        name="final",
    )


def fold_kernel(in_ref, out_ref):
    total = in_ref[0]
    for e in range(1, in_ref.shape[0]):
        total = total + in_ref[e]
    for e in range(out_ref.shape[0]):
        out_ref[e] = total


def call(kernel, outs, count=0):
    more = {}
    if count:
        more["in_specs"] = [pl.BlockSpec(memory_space=pltpu.SMEM)] + [pl.BlockSpec(memory_space=pltpu.VMEM)] * (count - 1)
    return pl.pallas_call(
        kernel,
        out_shape=[jax.ShapeDtypeStruct(s, d) for s, d in outs],
        compiler_params=pltpu.CompilerParams(vmem_limit_bytes=8 * 1024 * 1024),
        **more,
    )


WIDE = ((TOKENS, SPAN), lambda at: pl.BlockSpec((TOKENS, CHUNK * 128), lambda s, core: (0, at(s, core))))
WEIGHT = ((SPAN, 128), lambda at: pl.BlockSpec((CHUNK * 128, 128), lambda s, core: (at(s, core), 0)))
STATE = ((PAIRS * LANE_TOTAL, 128), lambda at: pl.BlockSpec((CHUNK * LANE_TOTAL, 128), lambda s, core: (at(s, core), 0)))
STATES = ((2, PAIRS * LANE_TOTAL, 128), lambda at: pl.BlockSpec((2, CHUNK * LANE_TOTAL, 128), lambda s, core: (0, at(s, core), 0)))


def whole(*shape):
    return (shape, lambda at: pl.BlockSpec(shape, lambda s, core: (0,) * len(shape)))


def kept(*shape):
    return (shape, lambda at: pl.BlockSpec(memory_space=pl.ANY))


TOTAL = ((STEPS, 2, CHUNK * 128), lambda at: pl.BlockSpec((1, 2, CHUNK * 128), lambda s, core: (at(s, core), 0, 0)))


def in_steps(kernel, ins, outs, scratch=(), at=lambda s, core: s, steps=STEPS, aliases=None, flops=10 ** 9):
    return pl.pallas_call(
        kernel,
        grid_spec=pltpu.PrefetchScalarGridSpec(
            num_scalar_prefetch=1,
            grid=(steps,),
            in_specs=[spec(at) for _, spec in ins],
            out_specs=[spec(at) for (_, spec), _ in outs],
            scratch_shapes=list(scratch),
        ),
        out_shape=[jax.ShapeDtypeStruct(shape, dtype) if shape in FREE else pltpu.HBM(shape, dtype) for (shape, spec), dtype in outs],
        compiler_params=pltpu.CompilerParams(vmem_limit_bytes=VMEM_LIMIT * 1024 * 1024, dimension_semantics=("arbitrary",)),
        cost_estimate=pl.CostEstimate(flops=flops, bytes_accessed=flops // 1000, transcendentals=0),
        input_output_aliases=aliases or {},
    )


ROWS = whole(PAIRS, 128)
SQUARE = whole(TOKENS, 128)
PART = whole(2 * HALF_ROWS + 16, 128)
STATE_PART = whole(2 * HALF_ROWS, 128)
HALF_WIDE = ((TOKENS, SPAN // 2), lambda at: pl.BlockSpec((TOKENS, CHUNK * 128), lambda s, core: (0, s)))
EARLY = [(WIDE, F32), (WIDE, BF16), (WIDE, BF16), (STATE, F32), (STATES, F32), (TOTAL, F32)]
SLOPE = [WIDE, WIDE, WIDE, TOTAL, WIDE, WIDE, STATE, STATES, STATE_PART, WIDE]


def mine_half(s, core):
    return core[0] * HALF_STEPS + s


def their_half(s, core):
    return (1 - core[0]) * HALF_STEPS + s


def theirs_call():
    return in_steps(
        theirs_kernel, [whole(TOKENS, SPAN), whole(SPAN, 128), WIDE, WIDE, WIDE, WIDE, WEIGHT, ROWS],
        [(SQUARE, F32)] + EARLY + [(PART, F32)], at=their_half, steps=HALF_STEPS,
    )


def mine_call():
    return in_steps(
        mine_kernel, [SQUARE, WIDE, WIDE, WIDE, WIDE, WEIGHT, ROWS] + [kept(*z[0][0]) for z in EARLY],
        EARLY + [(PART, F32)], at=mine_half, steps=HALF_STEPS, aliases={8 + j: j for j in range(len(EARLY))},
    )


def near_call():
    return in_steps(near_kernel, [WIDE] * 4 + [ROWS, WIDE], [(WIDE, F32)] * 5 + [(ROWS, F32)])


def slope_call():
    return in_steps(slope_kernel, SLOPE, [(HALF_WIDE, BF16), (whole(HALF, 128), F32)], at=mine_half, steps=HALF_STEPS)


def grads_call():
    return in_steps(
        grads_kernel, SLOPE + [whole(TOKENS, SPAN), whole(SPAN, 128), SQUARE, whole(TOKENS, SPAN // 2), whole(HALF, 128), ROWS],
        [(kept(32, 2, 48, 128), F32), (kept(32, 2, 48, 128), F32), (SQUARE, BF16)],
        (pltpu.VMEM((2, 2, SPAN // 2, 128), F32), pltpu.VMEM((2, 2, HALF, 8, 128), F32), pltpu.VMEM((TOKENS, 128), F32),
         pltpu.SemaphoreType.DMA((2, 2, 2))),
        at=their_half, steps=HALF_STEPS,
    )


def last_call():
    return in_steps(
        last_kernel,
        [WIDE, WIDE, WEIGHT, WIDE, WIDE, WIDE, STATE, STATES, STATE_PART, STATE_PART, WIDE, WIDE, WIDE, WIDE, SQUARE],
        [(WIDE, BF16)] * 5,
    )


def exchange(x, axes):
    return lax.all_to_all(x, axes, 0, 0, tiled=True)


def swap(x):
    return lax.ppermute(x, CORE, [(0, 1), (1, 0)])


def far(*arrays):
    return [pltpu.with_memory_space_constraint(z, pltpu.HBM) for z in arrays]


def inside(r, k, v, x, g, down, up, speed, bonus):
    r, k, v, x, g = (z[0] for z in (r, k, v, x, g))
    speed = speed.reshape(PAIRS, 128)
    bonus = bonus.reshape(PAIRS, 128)
    r, k, v, x, g, down, up, speed, bonus = far(r, k, v, x, g, down, up, speed, bonus)
    core = lax.axis_index(CORE).astype(jnp.int32)[None]
    flip = (lax.axis_index(CHIPS) // 16).astype(jnp.int32)[None]
    smooth, *early, theirs = theirs_call()(core, x, down, r, k, v, g, up, speed)
    (smooth,) = far(smooth)
    other = swap(theirs)
    *early, mine = mine_call()(core, smooth, r, k, v, g, up, speed, *far(*early))
    log_decay, reached, faded, own, pull, total = far(*early)
    (joined,) = call(join_kernel, [((32, 48, 128), F32)], 3)(core, mine, other)
    there = exchange(joined, CHIPS)
    near = near_call()(core, r, k, v, g, bonus, log_decay)
    fade, near_mixed, near_gr, near_gk, near_gv, bonus_rows = far(*near)
    (scanned,) = call(scan_kernel, [((32, 40, 128), F32)], 2)(flip, there)
    chip = exchange(scanned, CHIPS).reshape(2 * HALF_ROWS, 128)
    keep, give = call(part_kernel, [((2 * HALF_ROWS, 128), F32)] * 2, 4)(core, chip, mine, other)
    got = swap(give)
    slope_mine, sums_mine = far(*slope_call()(core, v, g, log_decay, total, reached, faded, own, pull, keep, fade))
    held, given, project_grad = grads_call()(core, v, g, log_decay, total, reached, faded, own, pull, got, fade,
                                             x, up, smooth, slope_mine, sums_mine, bonus_rows)
    (project_grad,) = far(project_grad)
    grads = (held + swap(given)).reshape(64, 48, 128)
    pieces = exchange(grads, CHIPS + ("dp",))
    mixed, gr, gk, gv, gx = last_call()(core, v, g, down, log_decay, reached, faded, own, pull, keep, got,
                                        near_mixed, near_gr, near_gk, near_gv, project_grad)
    (summed,) = call(fold_kernel, [((32, 48, 128), F32)])(pieces)
    matrix = exchange(summed, CHIPS)
    a, b, a_row, b_row = final_call()(core, matrix, swap(matrix))
    return (mixed[None], gr[None], gk[None], gv[None], gx[None],
            a.reshape(SPAN // 2, 128), b.reshape(SPAN // 2, 128), a_row.reshape(SPAN // 2), b_row.reshape(SPAN // 2))


def solution(mesh):
    split = Mesh(mesh.devices.reshape(4, 2, 4, 2, mesh.shape["dp"]), SEQ + ("dp",))
    tokens = P("dp", SEQ, None)
    return jax.shard_map(
        inside,
        mesh=split,
        in_specs=(tokens,) * 5 + (P(),) * 4,
        out_specs=(tokens,) * 5 + (P("dp", None), P("dp", None), P("dp"), P("dp")),
        check_vma=False,
    )
```
